32 devices in a mesh: dp: 2 (over x), expert: 16 (over z, y, core).
Axes of the slice: x: 2, y: 2, z: 4, core: 2. Of those that a mesh axis runs over, the one named last changes fastest.
Arguments:
- tokens: bfloat16 [4096, 2880], P('expert'), may hold values from -2 to 2
- segment_ids: int32 [4096], P('expert'), may hold values from 0 to 31, never falling along the last dimension, each value on 1 to 512 neighbouring positions
- expert_ids: int32 [4096, 4], P('expert'), may hold values from 0 to 15, as said below
- attn_gain: float32 [2880], replicated, may hold values from 0.1 to 1.9
- sinks: float32 [32], P('dp'), may hold values from 2 to 5
- qkv_master: float32 [2560, 2880], P(('dp', 'expert')), may hold values from -0.109375 to 0.109375
- qkv_mom: float32 [2560, 2880], P(('dp', 'expert')), may hold values from -0.006 to 0.006
- qkv_var: float32 [2560, 2880], P(('dp', 'expert')), may hold values from 1e-08 to 1e-06
- qkv_grad: float32 [2560, 2880], P(('dp', 'expert')), may hold values from -0.06 to 0.06
- o_master: float32 [2048, 2880], P(('dp', 'expert')), may hold values from -0.125 to 0.125
- o_mom: float32 [2048, 2880], P(('dp', 'expert')), may hold values from -0.006 to 0.006
- o_var: float32 [2048, 2880], P(('dp', 'expert')), may hold values from 1e-08 to 1e-06
- o_grad: float32 [2048, 2880], P(('dp', 'expert')), may hold values from -0.06 to 0.06
- router_weight: bfloat16 [2880, 16], replicated, may hold values from -0.109375 to 0.109375
- router_bias: float32 [16], replicated, may hold values from -4 to 4
- mlp_gain: float32 [2880], replicated, may hold values from 0.1 to 1.9
Outputs:
- dispatched: bfloat16 [16, 16, 2, 64, 2880], P('expert', None, 'dp')
- gate_slots: bfloat16 [16, 16, 2, 64], P('expert', None, 'dp')
The draws below stay inside these ranges and needn't reach their ends.
Inputs may be any that keep to these rules, and one draw needn't show every extreme that they name: `expert_ids`: each row names 4 different experts. In each aligned block of 128 rows no expert is named more than 64 times, and one expert, the same in every block of a draw, is named exactly 64 times in every block.
All inputs are finite; a program needn't handle non-finite values.
Results may differ from the reference program's by a relative error of at most 0.012.
The reference program's roundings to bfloat16 on the way count: a program that leaves them out, or rounds other values in their place, can miss the bound.
Values may be sent and summed in bfloat16 or wider, within the bound.
A program may use at most 128 MiB of HBM per device.

```python
import math
import jax
import jax.numpy as jnp
import numpy as np
from jax import lax

D = 2880
HEADS = 32
KV_HEADS = 4
HEAD_DIM = 64
WINDOW = 128
TOPK = 4
TOK_DEV = 256
EXPERTS = 16
TOKENS = 4096
BLOCK = 128
CAP = 64
QKV_ROWS = 2560
O_ROWS = 2048
N_DP = 2
N_EXPERT = 16


def draw_expert_ids(key, part):
    blocks = TOKENS // BLOCK
    pair_half = EXPERTS // 2
    base_key = jax.random.fold_in(key, 11)
    chosen = jax.random.randint(jax.random.fold_in(base_key, 1), (), 0, EXPERTS).astype(jnp.int32)

    def one_block(index):
        block_key = jax.random.fold_in(base_key, index + 7)
        ordering = jax.random.permutation(jax.random.fold_in(block_key, 1), EXPERTS).astype(jnp.int32)
        shares = jax.random.randint(jax.random.fold_in(block_key, 2), (pair_half,), 0, CAP + 1).astype(jnp.int32)
        where_pos = jnp.argmax(ordering == chosen).astype(jnp.int32)
        pair_pos = where_pos % pair_half
        forced = jnp.where(where_pos < pair_half, CAP, 0).astype(jnp.int32)
        shares = jnp.where(jnp.arange(pair_half, dtype=jnp.int32) == pair_pos, forced, shares)
        counts = jnp.zeros((EXPERTS,), jnp.int32).at[ordering].set(jnp.concatenate([shares, CAP - shares]))
        bounds = jnp.cumsum(counts)
        listing = jnp.searchsorted(bounds, jnp.arange(BLOCK * TOPK, dtype=jnp.int32), side='right').astype(jnp.int32)
        layout = listing.reshape(TOPK, BLOCK).T
        shuffle = jax.random.permutation(jax.random.fold_in(block_key, 3), BLOCK)
        return layout[shuffle]
    return jax.vmap(one_block)(jnp.arange(blocks, dtype=jnp.int32)).reshape(TOKENS, TOPK).astype(jnp.int32)


def block_levels(own_key, extent, cuts, least, top_value):
    factor_of = 1.0
    for dim, shards_of in cuts:
        heights = jax.random.uniform(jax.random.fold_in(jax.random.fold_in(own_key, 6), dim), (shards_of,), jnp.float32, least / len(cuts), top_value / len(cuts))
        factor_of = factor_of * jnp.repeat(jnp.exp(heights), extent[dim] // shards_of).reshape((-1,) + (1,) * (len(extent) - 1 - dim))
    return factor_of


def split_up(amount, total, reach, lean):
    weights = [(1 << 20) // math.isqrt(standing ** lean) + 1 for standing in range(2, amount + 1)]
    spare, given = total - reach - (amount - 1), [1] * (amount - 1)
    while spare > 0:
        candidates = [i for i in range(amount - 1) if given[i] < reach]
        mass, left = sum([weights[i] for i in candidates]), spare
        for i in candidates:
            extra = min(reach - given[i], max(1, left * weights[i] // mass), spare)
            given[i] = given[i] + extra
            spare = spare - extra
    return np.array([reach] + given)


def ragged_sizes(own_key, count, total, bound, skew):
    if count == 2:
        one = jax.random.randint(own_key, (), max(1, total - bound), min(bound, total - 1) + 1)
        return jnp.stack([one, total - one])
    tallies = jnp.asarray(split_up(count, total, bound, skew), jnp.int32)
    couples = (count - 1) // 2
    donor, sink = tallies[1:1 + 2 * couples:2], tallies[2:2 + 2 * couples:2]
    room = jnp.minimum(donor - 1, bound - sink)
    shifted = jax.random.randint(jax.random.fold_in(own_key, 1), (couples,), 0, 1 << 20) % (room + 1)
    tallies = tallies.at[1:1 + 2 * couples:2].set(donor - shifted).at[2:2 + 2 * couples:2].set(sink + shifted)
    return tallies[jax.random.permutation(jax.random.fold_in(own_key, 2), count)]


def noise(rng, dims, deviation, bound, split=(), kind=jnp.bfloat16):
    array = deviation * jax.random.normal(rng, dims, jnp.float32)
    if split:
        array = array * block_levels(rng, dims, split, -0.22, 0.18)
    return jnp.clip(array, -bound, bound).astype(kind)


def setup_inputs(seed: int = 0) -> dict:
    key_list = jax.random.split(jax.random.key(seed), 17)
    tokens = noise(key_list[0], (TOKENS, D), 0.3, 2.0, ((0, 16),))
    segment_ids = jnp.searchsorted(jnp.cumsum(ragged_sizes(key_list[1], TOKENS // 128, TOKENS, 512, 1)), jnp.arange(TOKENS), side="right").astype(jnp.int32)
    expert_ids = draw_expert_ids(jax.random.fold_in(key_list[16], 71), 0)
    attn_gain = jnp.clip(1.0 + 0.18 * jax.random.normal(key_list[3], (D,), jnp.float32), 0.1, 1.9)
    sinks = jnp.clip(2.0 + 3.0 * jax.random.uniform(key_list[4], (HEADS,), jnp.float32) ** block_levels(key_list[4], (HEADS,), ((0, 2),), -0.2, 0.2), 2.0, 5.0)
    qkv_master = noise(key_list[5], (QKV_ROWS, D), D ** -0.5, 0.109375, ((0, 32),), jnp.float32)
    qkv_mom = noise(key_list[6], (QKV_ROWS, D), 0.001, 0.006, ((0, 32),), jnp.float32)
    qkv_var = jnp.clip(jnp.exp(math.log(9.999999974752427e-07) - 4.6051702 * jax.random.uniform(key_list[7], (QKV_ROWS, D), jnp.float32) ** block_levels(key_list[7], (QKV_ROWS, D), ((0, 32),), -0.2, 0.2)), 9.99999993922529e-09, 9.999999974752427e-07)
    qkv_grad = noise(key_list[8], (QKV_ROWS, D), 0.01, 0.06, ((0, 32),), jnp.float32)
    o_master = noise(key_list[9], (O_ROWS, D), O_ROWS ** -0.5, 0.125, ((0, 32),), jnp.float32)
    o_mom = noise(key_list[10], (O_ROWS, D), 0.001, 0.006, ((0, 32),), jnp.float32)
    o_var = jnp.clip(jnp.exp(math.log(9.999999974752427e-07) - 4.6051702 * jax.random.uniform(key_list[11], (O_ROWS, D), jnp.float32) ** block_levels(key_list[11], (O_ROWS, D), ((0, 32),), -0.2, 0.2)), 9.99999993922529e-09, 9.999999974752427e-07)
    o_grad = noise(key_list[12], (O_ROWS, D), 0.01, 0.06, ((0, 32),), jnp.float32)
    router_weight = noise(key_list[13], (D, EXPERTS), D ** -0.5, 0.109375)
    router_bias = noise(key_list[14], (EXPERTS,), 1.0, 4.0, (), jnp.float32)
    mlp_gain = jnp.clip(1.0 + 0.18 * jax.random.normal(key_list[15], (D,), jnp.float32), 0.1, 1.9)
    return dict(tokens=tokens, segment_ids=segment_ids, expert_ids=expert_ids, attn_gain=attn_gain, sinks=sinks, qkv_master=qkv_master, qkv_mom=qkv_mom, qkv_var=qkv_var, qkv_grad=qkv_grad, o_master=o_master, o_mom=o_mom, o_var=o_var, o_grad=o_grad, router_weight=router_weight, router_bias=router_bias, mlp_gain=mlp_gain)


beta_one = 0.9
beta_two = 0.999
adam_step = 100
learn_rate = 0.02
adam_eps = 1e-08
norm_eps = 1e-05
rope_base = 150000.0
contract_rows = (((1,), (1,)), ((), ()))

def adam_weights(master, moment, second_mom, gradient):
    moment_new = beta_one * moment + (1.0 - beta_one) * gradient
    second_new = beta_two * second_mom + (1.0 - beta_two) * gradient * gradient
    fix_one = 1.0 - beta_one ** adam_step
    fix_two = 1.0 - beta_two ** adam_step
    update = moment_new / fix_one / (jnp.sqrt(second_new / fix_two) + adam_eps)
    return (master - learn_rate * update).astype(jnp.bfloat16)

def rms_scale(values, gain_vec):
    mean_sq = lax.optimization_barrier(jnp.mean(values * values, axis=-1, keepdims=True))
    return values * lax.rsqrt(mean_sq + norm_eps) * gain_vec

def rotate(values, positions):
    half_dim = values.shape[-1] // 2
    frequency = rope_base ** (-(jnp.arange(half_dim).astype(jnp.float32) * 2.0) / values.shape[-1])
    angles = positions[:, None] * frequency[None, :]
    cosine = jnp.cos(angles)[:, None, :]
    sine_vals = jnp.sin(angles)[:, None, :]
    first_half = values[..., :half_dim]
    second_half = values[..., half_dim:]
    return jnp.concatenate([first_half * cosine - second_half * sine_vals, second_half * cosine + first_half * sine_vals], axis=-1)

def attention(queries, key_rows, value_rows, segments, sink_logits):
    row_count = queries.shape[0]
    scale = queries.shape[-1] ** (-0.5)
    scores = jnp.einsum('tgrd,ugd->grtu', queries.astype(jnp.float32), key_rows.astype(jnp.float32)) * scale
    position = jnp.arange(row_count, dtype=jnp.int32)
    offset = position[:, None] - position[None, :]
    allowed = (segments[:, None] == segments[None, :]) & (offset >= 0) & (offset < WINDOW)
    weights = jnp.where(allowed, jnp.exp(scores), 0.0)
    sink_terms = jnp.exp(sink_logits).reshape(key_rows.shape[1], -1)[:, :, None]
    running = sink_terms + lax.optimization_barrier(jnp.sum(weights, axis=-1))
    attn_probs = (weights / running[..., None]).astype(jnp.bfloat16)
    attended = jnp.einsum('grtu,ugd->tgrd', attn_probs.astype(jnp.float32), value_rows.astype(jnp.float32))
    return attended.astype(jnp.bfloat16).reshape(row_count, -1)

def gate_values(logits, choices, experts):
    picked = choices[:, :, None] == jnp.arange(experts, dtype=jnp.int32)[None, None, :]
    chosen = lax.optimization_barrier(jnp.sum(jnp.where(picked, logits[:, None, :], 0.0), axis=-1))
    raised = jnp.exp(chosen)
    return raised / lax.optimization_barrier(jnp.sum(raised, axis=-1, keepdims=True))

def slot_targets(choices, capacity, experts):
    flat_ids = choices.reshape(-1).astype(jnp.int32)
    onehot = (flat_ids[:, None] == jnp.arange(experts, dtype=jnp.int32)[None, :]).astype(jnp.int32)
    earlier = jnp.cumsum(onehot, axis=0) - onehot
    slot_index = lax.optimization_barrier(jnp.sum(earlier * onehot, axis=1)).astype(jnp.int32)
    return flat_ids * capacity + slot_index

def reference(tokens, segment_ids, expert_ids, attn_gain, sinks, qkv_master, qkv_mom, qkv_var, qkv_grad, o_master, o_mom, o_var, o_grad, router_weight, router_bias, mlp_gain):
    qkv_weight = adam_weights(qkv_master, qkv_mom, qkv_var, qkv_grad)
    o_weight = adam_weights(o_master, o_mom, o_var, o_grad)
    group_rows = QKV_ROWS // N_DP
    q_rows = HEADS // N_DP * HEAD_DIM
    kv_rows = KV_HEADS // N_DP * HEAD_DIM
    repeat_count = HEADS // KV_HEADS
    positions = jnp.arange(TOK_DEV).astype(jnp.float32)

    def per_pack(pack_data):
        rows, segments, choices = pack_data
        normed = rms_scale(rows.astype(jnp.float32), attn_gain).astype(jnp.bfloat16)
        projected = lax.dot_general(normed, qkv_weight, contract_rows, preferred_element_type=jnp.float32)
        projected = projected.reshape(TOK_DEV, N_DP, group_rows)
        queries = rotate(projected[:, :, :q_rows].reshape(TOK_DEV, HEADS, HEAD_DIM), positions).astype(jnp.bfloat16)
        queries = queries.reshape(TOK_DEV, KV_HEADS, repeat_count, HEAD_DIM)
        key_rows = rotate(projected[:, :, q_rows:q_rows + kv_rows].reshape(TOK_DEV, KV_HEADS, HEAD_DIM), positions).astype(jnp.bfloat16)
        value_rows = projected[:, :, q_rows + kv_rows:].reshape(TOK_DEV, KV_HEADS, HEAD_DIM).astype(jnp.bfloat16)
        attended = attention(queries, key_rows, value_rows, segments, sinks)
        residual = rows.astype(jnp.float32) + jnp.dot(attended, o_weight, preferred_element_type=jnp.float32)
        moe_all = rms_scale(residual, mlp_gain).astype(jnp.bfloat16)
        payloads = []
        gate_lists = []
        for group_num in range(N_DP):
            row_start = group_num * BLOCK
            moe_in = moe_all[row_start:row_start + BLOCK]
            block_ids = choices[row_start:row_start + BLOCK]
            logits = jnp.dot(moe_in, router_weight, preferred_element_type=jnp.float32) + router_bias
            gate_vals = gate_values(logits, block_ids, EXPERTS)
            target = slot_targets(block_ids, CAP, EXPERTS)
            source_row = jnp.arange(BLOCK * TOPK, dtype=jnp.int32) // TOPK
            payload = jnp.zeros((EXPERTS * CAP, D), jnp.bfloat16).at[target].set(moe_in[source_row])
            slot_gates = jnp.zeros((EXPERTS * CAP,), jnp.bfloat16).at[target].set(gate_vals.reshape(-1).astype(jnp.bfloat16))
            payloads.append(payload.reshape(EXPERTS, CAP, D))
            gate_lists.append(slot_gates.reshape(EXPERTS, CAP))
        return (jnp.stack(payloads), jnp.stack(gate_lists))
    packed = (tokens.reshape(N_EXPERT, TOK_DEV, D), segment_ids.reshape(N_EXPERT, TOK_DEV), expert_ids.reshape(N_EXPERT, TOK_DEV, TOPK))
    payload_all, gates_all = lax.map(per_pack, packed)
    dispatched = jnp.transpose(payload_all, (2, 0, 1, 3, 4))
    gate_slots = jnp.transpose(gates_all, (2, 0, 1, 3))
    return (dispatched, gate_slots)
```

```python
import functools
import types

import jax
import jax.numpy as jnp
import numpy as np
from jax import lax
from jax.experimental import pallas as pl
from jax.experimental.pallas import tpu as pltpu
from jax.sharding import PartitionSpec as P

HEADS = 32
KV_HEADS = 4
HEAD_DIM = 64
WINDOW = 128
MESH = pl.DeviceIdType.MESH
VMEM_BYTES = 36 * 1024 * 1024


beta_one = 0.9
beta_two = 0.999
adam_step = 100
learn_rate = 0.02
adam_eps = 1e-08
norm_eps = 1e-05
rope_base = 150000.0


def adam_weights(master, moment, second_mom, gradient):
    moment_new = beta_one * moment + (1.0 - beta_one) * gradient
    second_new = beta_two * second_mom + (1.0 - beta_two) * gradient * gradient
    fix_one = 1.0 - beta_one**adam_step
    fix_two = 1.0 - beta_two**adam_step
    update = moment_new / fix_one / (jnp.sqrt(second_new / fix_two) + adam_eps)
    return (master - learn_rate * update).astype(jnp.bfloat16)


def rotation_tables(rows):
    half_dim = HEAD_DIM // 2
    positions = jnp.arange(rows).astype(jnp.float32)
    frequency = rope_base ** (-(jnp.arange(half_dim).astype(jnp.float32) * 2.0) / HEAD_DIM)
    angles = positions[:, None] * frequency[None, :]
    cosine = jnp.cos(angles)
    sine = jnp.sin(angles)
    return (
        jnp.concatenate([cosine] * 4, axis=1),
        jnp.concatenate([-sine, sine, -sine, sine], axis=1),
    )


def chip_at(place, chips):
    place = lax.rem(place + 2 * chips, chips)
    return jnp.where(place < chips // 2, 2 * place, 2 * (chips - 1 - place) + 1)


def gather_kernel(chips, plan, top_count, *refs):
    count = len({entry[0] for entry in plan})
    if top_count:
        (source, out_ref, gate_ref, held), sems = refs[:4], refs[4:]
        ins, outs = (source,), (held,)
    else:
        ins, outs, sems = refs[:count], refs[count : 2 * count], refs[2 * count :]
    ring_send, ring_recv, pair_send, pair_recv, own_send, own_recv, own_sem = sems
    me = lax.axis_index("expert")
    core = lax.rem(me, 2)
    chip = me // 2
    place = jnp.where(lax.rem(chip, 2) == 0, chip // 2, chips - 1 - chip // 2)
    right = chip_at(place + 1, chips) * 2 + core
    left = chip_at(place - 1, chips) * 2 + core
    partner = me + 1 - 2 * core

    barrier = pltpu.get_barrier_semaphore()
    for other in (left, right, partner):
        pl.semaphore_signal(barrier, inc=1, device_id={"expert": other}, device_id_type=MESH)
    pl.semaphore_wait(barrier, 3)

    def block(j, slot):
        arr, start, size = plan[j][:3]
        return outs[arr].at[slot, pl.ds(start, size)]

    def origin(way, step):
        return chip_at(place - step if way > 0 else place + step, chips) * 2 + core

    def copy_to(j, step, send, recv, target):
        arr, start, size, way, _ = plan[j]
        slot = origin(way, step)
        return pltpu.make_async_remote_copy(
            src_ref=ins[arr].at[pl.ds(start, size)] if step == 0 else block(j, slot),
            dst_ref=block(j, slot),
            send_sem=send.at[j, step],
            recv_sem=recv.at[j, step],
            device_id={"expert": target},
            device_id_type=MESH,
        )

    def ring_copy(j, step):
        return copy_to(j, step, ring_send, ring_recv, right if plan[j][3] > 0 else left)

    def pair_copy(j, step):
        return copy_to(j, step, pair_send, pair_recv, partner)

    def own_copy(arr, slot):
        return pltpu.make_async_remote_copy(
            src_ref=ins[arr],
            dst_ref=outs[arr].at[slot],
            send_sem=own_send.at[arr],
            recv_sem=own_recv.at[arr],
            device_id={"expert": partner},
            device_id_type=MESH,
        )

    def landed(j, slot, sem):
        pltpu.make_async_copy(block(j, slot), block(j, slot), sem).wait()

    def consume(rows, slot):
        if top_count:
            fill_slots(top_count, rows, out_ref, gate_ref, slot)

    def take_mine():
        consume(ins[0], me)

    def take_partner():
        for arr in range(count):
            pltpu.make_async_copy(
                outs[arr].at[partner], outs[arr].at[partner], own_recv.at[arr]
            ).wait()
        consume(outs[0].at[partner], partner)

    def take_ring(way, step):
        slot = origin(way, step)
        consume(outs[0].at[slot], slot)

    def take_pair(ways, step):
        for j, entry in enumerate(plan):
            if entry[3] in ways and step <= entry[4]:
                landed(j, origin(entry[3], step) + 1 - 2 * core, pair_recv.at[j, step])
        slot = origin(ways[0], step) + 1 - 2 * core
        consume(outs[0].at[slot], slot)

    every = range(len(plan))
    hops = chips // 2
    for j in every:
        ring_copy(j, 0).start()
    for arr in range(count):
        own_copy(arr, me).start()
    owns = []
    if not top_count:
        owns = [
            pltpu.make_async_copy(ins[a], outs[a].at[me], own_sem.at[a]) for a in range(count)
        ]
    for copy in owns:
        copy.start()
    tasks = [take_mine, take_partner]
    for step in range(1, hops + 1):
        for j in every:
            if step > plan[j][4]:
                continue
            landed(j, origin(plan[j][3], step), ring_recv.at[j, step - 1])
            if step < plan[j][4]:
                ring_copy(j, step).start()
            pair_copy(j, step).start()
            if tasks:
                tasks.pop(0)()
        for ways in ((1,), (-1,)) if step < hops else ((1, -1),):
            tasks.append(functools.partial(take_ring, ways[0], step))
            tasks.append(functools.partial(take_pair, ways, step))
    tasks = tasks[::2] + tasks[1::2]
    for task in tasks:
        task()
    for copy in owns:
        copy.wait()
    for arr in range(count):
        own_copy(arr, me).wait_send()
    for j in every:
        for step in range(plan[j][4] + 1):
            if step:
                pair_copy(j, step).wait_send()
            if step < plan[j][4]:
                ring_copy(j, step).wait_send()


def ring_gather(arrays, cuts, sources, call_id, slots=None):
    plan = []
    chips = sources // 2
    for arr, value in enumerate(arrays):
        tiles = value.shape[0] // 16
        for cut in range(cuts):
            start = (tiles * cut + cuts - 1) // cuts * 16
            size = (tiles * (cut + 1) + cuts - 1) // cuts * 16 - start
            for way in (1, -1):
                far = (cut < cuts // 2) == (way > 0)
                plan.append((arr, start, size, way, chips // 2 - (0 if far else 1)))
    copies, count = len(plan), len(arrays)
    gathered = [jax.ShapeDtypeStruct((sources, *v.shape), v.dtype) for v in arrays]
    sems = [pltpu.SemaphoreType.DMA((copies, chips // 2 + 1))] * 4
    sems += [pltpu.SemaphoreType.DMA((count,))] * 3
    vmem = pl.BlockSpec(memory_space=pltpu.VMEM)
    if slots:
        top_count, capacity, width = slots
        out_shape = (
            jax.ShapeDtypeStruct((sources, capacity, width), jnp.bfloat16),
            jax.ShapeDtypeStruct((sources, 1, capacity), jnp.bfloat16),
        )
        out_specs = (vmem, vmem)
        held = [pltpu.VMEM(gathered[0].shape, gathered[0].dtype)]
    else:
        top_count, out_shape, held = 0, gathered, []
        out_specs = [vmem] * count
    return pl.pallas_call(
        functools.partial(gather_kernel, chips, tuple(plan), top_count),
        out_shape=out_shape,
        in_specs=[vmem] * count,
        out_specs=out_specs,
        scratch_shapes=held + sems,
        compiler_params=pltpu.CompilerParams(
            collective_id=call_id, has_side_effects=True,
            vmem_limit_bytes=(40 if slots else 24) * 1024 * 1024,
        ),
        name="ring_slots" if slots else "ring_gather",
    )(*arrays)


def ring_fits(arrays, sources):
    return sources % 4 == 0 and 8 <= sources <= 32 and all(a.shape[0] % 16 == 0 for a in arrays)


def gather_rows(arrays, sources, call_id):
    if ring_fits(arrays, sources):
        width = arrays[0].shape[1]
        return [v.reshape(-1, width) for v in ring_gather(arrays, 2, sources, call_id)]
    return [lax.all_gather(a, "expert", axis=0, tiled=True) for a in arrays]


def swap_halves(values, lane):
    up = pltpu.roll(values, 128 - HEAD_DIM // 2, 1)
    down = pltpu.roll(values, HEAD_DIM // 2, 1)
    return jnp.where(lane % HEAD_DIM < HEAD_DIM // 2, up, down)


def attention_kernel(
    heads, kv_heads, tok_ref, gain_ref, w_ref, o_ref, cos_ref, sin_ref, seg_col, seg_row, sink_ref,
    out_ref, proj_ref, att_ref,
):
    rows = tok_ref.shape[0]
    bf16 = jnp.bfloat16
    values = tok_ref[...].astype(jnp.float32)
    mean_sq = jnp.mean(values * values, axis=-1, keepdims=True)
    normed = (values * lax.rsqrt(mean_sq + norm_eps) * gain_ref[...][None, :]).astype(bf16)
    features = w_ref.shape[0]
    for start in range(0, features, 256):
        size = min(256, features - start)
        proj_ref[:, start : start + size] = lax.dot_general(
            normed, w_ref[start : start + size, :], (((1,), (1,)), ((), ())),
            preferred_element_type=jnp.float32,
        )
    lane = lax.broadcasted_iota(jnp.int32, (rows, 128), 1)
    low = lane < HEAD_DIM
    cosine, sine = cos_ref[...], sin_ref[...]
    row = lax.broadcasted_iota(jnp.int32, (rows, rows), 0)
    col = lax.broadcasted_iota(jnp.int32, (rows, rows), 1)
    offset = row - col
    allowed = (seg_col[...] == seg_row[...]) & (offset >= 0) & (offset < WINDOW)
    q_rows = heads * HEAD_DIM
    kv_rows = kv_heads * HEAD_DIM
    repeat = heads // kv_heads
    zero = jnp.zeros((rows, 128), jnp.float32)
    for group in range(kv_heads):
        base = q_rows + group // 2 * 128
        keys = proj_ref[:, base : base + 128]
        keys = keys * cosine + swap_halves(keys, lane) * sine
        vals = proj_ref[:, base + kv_rows : base + kv_rows + 128]
        keys_turned, vals_turned = pltpu.roll(keys, HEAD_DIM, 1), pltpu.roll(vals, HEAD_DIM, 1)
        if group % 2 == 1:
            keys, keys_turned, vals, vals_turned = keys_turned, keys, vals_turned, vals
        sides = (
            (jnp.where(low, keys, zero).astype(bf16), jnp.where(low, vals, zero).astype(bf16)),
            (
                jnp.where(low, zero, keys_turned).astype(bf16),
                jnp.where(low, zero, vals_turned).astype(bf16),
            ),
        )
        for slab in range(group * repeat // 2, (group + 1) * repeat // 2):
            query = proj_ref[:, slab * 128 : slab * 128 + 128]
            query = (query * cosine + swap_halves(query, lane) * sine).astype(bf16)
            total = None
            for side, (key_side, val_side) in enumerate(sides):
                scores = lax.dot_general(
                    query, key_side, (((1,), (1,)), ((), ())), preferred_element_type=jnp.float32
                ) * (HEAD_DIM**-0.5)
                weights = jnp.where(allowed, jnp.exp(scores), 0.0)
                running = jnp.exp(jnp.full((rows, 1), sink_ref[2 * slab + side])) + jnp.sum(weights, axis=-1, keepdims=True)
                probs = (weights * (1.0 / running)).astype(bf16)
                part = jnp.dot(probs, val_side, preferred_element_type=jnp.float32)
                total = part if total is None else total + part
            att_ref[:, slab * 128 : slab * 128 + 128] = total.astype(bf16)
    width = o_ref.shape[1]
    for start in range(0, width, 384):
        size = min(384, width - start)
        out_ref[:, start : start + size] = jnp.dot(
            att_ref[...], o_ref[:, start : start + size], preferred_element_type=jnp.float32
        ).astype(bf16)


def attention_call(tokens, gain, qkv_full, o_full, segments, sinks, heads, kv_heads):
    rows, width = tokens.shape
    cosine, sine = rotation_tables(rows)
    vmem = pl.BlockSpec(memory_space=pltpu.VMEM)
    return pl.pallas_call(
        functools.partial(attention_kernel, heads, kv_heads),
        out_shape=jax.ShapeDtypeStruct((rows, width), jnp.bfloat16),
        in_specs=[vmem] * 8 + [pl.BlockSpec(memory_space=pltpu.SMEM)],
        out_specs=vmem,
        scratch_shapes=[
            pltpu.VMEM((rows, qkv_full.shape[0]), jnp.float32),
            pltpu.VMEM((rows, heads * HEAD_DIM), jnp.bfloat16),
        ],
        compiler_params=pltpu.CompilerParams(vmem_limit_bytes=VMEM_BYTES),
        name="attention_part",
    )(
        tokens, gain, qkv_full, o_full, cosine, sine, segments[:, None],
        segments[None, :], sinks,
    )


def exchange_kernel(part_ref, got_ref, send_sem, recv_sem):
    group = lax.axis_index("dp")
    other = 1 - group
    barrier = pltpu.get_barrier_semaphore()
    pl.semaphore_signal(barrier, inc=1, device_id={"dp": other}, device_id_type=MESH)
    pl.semaphore_wait(barrier, 1)
    copy = pltpu.make_async_remote_copy(
        src_ref=part_ref.at[other],
        dst_ref=got_ref,
        send_sem=send_sem,
        recv_sem=recv_sem,
        device_id={"dp": other},
        device_id_type=MESH,
    )
    copy.start()
    copy.wait()


def exchange_call(part, call_id):
    return pl.pallas_call(
        exchange_kernel,
        out_shape=jax.ShapeDtypeStruct(part.shape[1:], part.dtype),
        in_specs=[pl.BlockSpec(memory_space=pltpu.VMEM)],
        out_specs=pl.BlockSpec(memory_space=pltpu.VMEM),
        scratch_shapes=[pltpu.SemaphoreType.DMA, pltpu.SemaphoreType.DMA],
        compiler_params=pltpu.CompilerParams(
            collective_id=call_id, has_side_effects=True, vmem_limit_bytes=16 * 1024 * 1024
        ),
        name="exchange_halves",
    )(part)


def router_kernel(tok_ref, part_ref, got_ref, gain_ref, rw_ref, bias_ref, ids_ref, out_ref):
    group = lax.axis_index("dp")
    half, width = got_ref.shape
    experts = rw_ref.shape[0]
    top_count = ids_ref.shape[1]
    rows = pl.ds(pl.multiple_of(group * half, half), half)
    summed = part_ref[group].astype(jnp.float32) + got_ref[...].astype(jnp.float32)
    residual = tok_ref[rows, :].astype(jnp.float32) + summed
    mean_sq = jnp.mean(residual * residual, axis=-1, keepdims=True)
    moe_in = (residual * lax.rsqrt(mean_sq + norm_eps) * gain_ref[...][None, :]).astype(jnp.bfloat16)
    out_ref[:, :width] = moe_in
    logits = lax.dot_general(
        moe_in, rw_ref[...], (((1,), (1,)), ((), ())), preferred_element_type=jnp.float32
    ) + bias_ref[...]
    ids = ids_ref[rows, :]
    expert = lax.broadcasted_iota(jnp.int32, (half, experts), 1)
    picked = [ids[:, k : k + 1] == expert for k in range(top_count)]
    hit = sum(jnp.where(p, 1.0, 0.0) for p in picked)
    above = lax.broadcasted_iota(jnp.int32, (half, half), 0) > lax.broadcasted_iota(
        jnp.int32, (half, half), 1
    )
    before = jnp.dot(
        jnp.where(above, 1.0, 0.0).astype(jnp.bfloat16), hit.astype(jnp.bfloat16),
        preferred_element_type=jnp.float32,
    )
    raised = [jnp.exp(jnp.sum(jnp.where(p, logits, 0.0), axis=1, keepdims=True)) for p in picked]
    scale = 1.0 / sum(raised)
    column = lax.broadcasted_iota(jnp.int32, (half, out_ref.shape[1] - width), 1)
    extra = jnp.zeros(column.shape, jnp.float32)
    for k in range(top_count):
        slot = jnp.sum(jnp.where(picked[k], before, 0.0), axis=1, keepdims=True)
        extra = jnp.where(column == 3 * k, raised[k] * scale, extra)
        extra = jnp.where(column == 3 * k + 1, ids[:, k : k + 1].astype(jnp.float32), extra)
        extra = jnp.where(column == 3 * k + 2, slot, extra)
    out_ref[:, width:] = extra.astype(jnp.bfloat16)


def router_call(tokens, part, got, gain, router_weight, router_bias, expert_ids, extra):
    half, width = got.shape
    return pl.pallas_call(
        router_kernel,
        out_shape=jax.ShapeDtypeStruct((half, width + extra), jnp.bfloat16),
        in_specs=[pl.BlockSpec(memory_space=pltpu.VMEM)] * 7,
        out_specs=pl.BlockSpec(memory_space=pltpu.VMEM),
        compiler_params=pltpu.CompilerParams(vmem_limit_bytes=VMEM_BYTES),
        name="router_part",
    )(tokens, part, got, gain, router_weight.T, router_bias[None, :], expert_ids)


def fill_slots(top_count, rows_ref, out_ref, gate_ref, slot):
    mine = lax.axis_index("expert").astype(jnp.float32)
    _, capacity, width = out_ref.shape
    half, full = rows_ref.shape
    extra = rows_ref[:, full - 128 :].astype(jnp.float32)
    shift = 128 - (full - width)
    place = lax.broadcasted_iota(jnp.int32, (half, capacity), 1).astype(jnp.float32)
    select = jnp.zeros((half, capacity), jnp.float32)
    gates = jnp.zeros((half, capacity), jnp.float32)
    for k in range(top_count):
        at = shift + 3 * k
        match = (extra[:, at + 1 : at + 2] == mine) & (extra[:, at + 2 : at + 3] == place)
        select = jnp.where(match, 1.0, select)
        gates = jnp.where(match, extra[:, at : at + 1], gates)
    gate_ref[slot] = jnp.sum(gates, axis=0, keepdims=True).astype(jnp.bfloat16)
    out_ref[slot] = lax.dot_general(
        select.astype(jnp.bfloat16), rows_ref[:, :width], (((0,), (0,)), ((), ())),
        preferred_element_type=jnp.float32,
    ).astype(jnp.bfloat16)


def exchange_slots(rows, width, experts, capacity, top_count, sources):
    half = rows.shape[0]
    extra = rows[:, width:].astype(jnp.float32)
    moe_in = rows[:, :width]
    gates, ids, slots = (extra[:, i : 3 * top_count : 3] for i in range(3))
    target = (ids * capacity + slots).astype(jnp.int32).reshape(-1)
    matches = target[None, :] == jnp.arange(experts * capacity, dtype=jnp.int32)[:, None]
    token_match = jnp.any(matches.reshape(experts * capacity, half, top_count), axis=2)
    payload = jnp.dot(
        token_match.astype(jnp.bfloat16), moe_in, preferred_element_type=jnp.float32
    ).astype(jnp.bfloat16)
    slot_gates = jnp.sum(jnp.where(matches, gates.reshape(-1)[None, :], 0.0), axis=1)
    outgoing = (
        payload.reshape(experts, capacity, width),
        slot_gates.astype(jnp.bfloat16).reshape(experts, capacity),
    )
    got_rows, got_gates = (
        lax.all_to_all(v, "expert", split_axis=0, concat_axis=0, tiled=True) for v in outgoing
    )
    per_device = experts // sources
    got_rows = got_rows.reshape(sources, per_device, capacity, width)
    got_gates = got_gates.reshape(sources, per_device, capacity)
    return (
        jnp.transpose(got_rows, (1, 0, 2, 3))[:, :, None],
        jnp.transpose(got_gates, (1, 0, 2))[:, :, None],
    )


def split_tables(rows):
    half_dim = HEAD_DIM // 2
    positions = np.arange(rows).astype(np.float64)
    powers = -(np.arange(half_dim).astype(np.float64) * 2.0) / HEAD_DIM
    frequency = (rope_base**powers).astype(np.float32).astype(np.float64)
    angles = (positions[:, None] * frequency[None, :]).astype(np.float32).astype(np.float64)
    cosine, sine = np.cos(angles), np.sin(angles)
    return (
        np.concatenate([cosine] * 4, axis=1).astype(np.float32),
        np.concatenate([-sine, sine, -sine, sine], axis=1).astype(np.float32),
    )


def piece_plan(groups, hops):
    plan, base = [], 0
    for group, spans in enumerate(groups):
        for start, size, far_way in spans:
            for way in (1, -1):
                count = hops if way == far_way else hops - 1
                plan.append((group, start, size, way, count, base))
                base += count
    return tuple(plan), base


def layer_kernel(cfg, hbm, r):
    bf16, f32 = jnp.bfloat16, jnp.float32
    chips, plan = cfg.chips, cfg.plan
    hops = chips // 2
    me = lax.axis_index("expert")
    side = lax.axis_index("dp")
    core = lax.rem(me, 2)
    chip = me // 2
    place = jnp.where(lax.rem(chip, 2) == 0, chip // 2, chips - 1 - chip // 2)
    right = chip_at(place + 1, chips) * 2 + core
    left = chip_at(place - 1, chips) * 2 + core
    flip = 1 - 2 * core
    partner = me + flip
    across = 1 - side
    rows, width = r.tok.shape
    half = rows // 2
    q_block = r.q_in.shape[1]
    o_block = r.o_in.shape[1]
    capacity = r.out.shape[1]
    cut = cfg.segments[0][1]

    names = []

    def load(name, pairs):
        for src, dst in pairs:
            pltpu.make_async_copy(src, dst, r.load_sem.at[len(names)]).start()
        names.append(name)

    def ready(name, ref):
        pltpu.make_async_copy(ref, ref, r.load_sem.at[names.index(name)]).wait()

    def tile_of(start):
        return r.q_in.at[:, pl.ds(start, 16)]

    for start in range(0, q_block, 16):
        part = pl.ds(start, 16)
        load(start, [(hbm.adam[i].at[part], r.q_in.at[i, part]) for i in range(4)])
    load("tok", [(hbm.tok, r.tok_t)])
    load("o", [(hbm.adam[4 + i], r.o_in.at[i]) for i in range(4)])
    for index, pair in enumerate(zip(hbm.small, r.small)):
        load(-1 - index, [pair])
    gain, mlp, seg_row, cosine, sine, router, bias, ids_ref, sinks = r.small

    barrier = pltpu.get_barrier_semaphore()
    for other in (left, right, partner):
        pl.semaphore_signal(barrier, inc=1, device_id={"expert": other}, device_id_type=MESH)
    pl.semaphore_signal(barrier, inc=1, device_id={"dp": across}, device_id_type=MESH)
    pl.semaphore_wait(barrier, 4)

    swaps = len(cfg.segments)
    fast, slow, marks = swaps + 2, swaps + 3, swaps + 4
    full = width // 128 * 128
    held = (r.w_q, r.tails, *r.o_part, r.rows_a, r.rows_b, r.notes)
    stride = (q_block, 0, *[o_block] * swaps, 0, 0, 0)

    def block(group, slot, start, size):
        ref = held[group]
        columns = pl.ds(0, ref.shape[-1] // 128 * 128)
        if stride[group]:
            first = pl.multiple_of(slot * stride[group] + start, 16)
            return ref.at[pl.ds(first, size), columns]
        return ref.at[slot, pl.ds(start, size), columns]

    def blocks(group, count):
        if stride[group]:
            return block(group, 0, 0, count * stride[group])
        columns = pl.ds(0, held[group].shape[-1] // 128 * 128)
        return held[group].at[pl.ds(0, count), :, columns]

    def origin(way, step):
        return chip_at(place - step if way > 0 else place + step, chips) * 2 + core

    def send(ref, device, out_sem, in_sem):
        return pltpu.make_async_remote_copy(
            src_ref=ref, dst_ref=ref, send_sem=out_sem, recv_sem=in_sem,
            device_id={"expert": device}, device_id_type=MESH,
        )

    def ring_copy(entry, step):
        group, start, size, way, _, base = entry
        return send(
            block(group, origin(way, step), start, size), right if way > 0 else left,
            r.ring_send.at[group], r.ring_recv.at[base + step],
        )

    def mark(group, way, step):
        if group < fast:
            return group
        at = fast + 2 * hops * (group - fast)
        return at if step == 0 else at + (2 * step - (way > 0) if step < hops else 2 * step - 1)

    def pair_copy(entry, step):
        group, start, size, way, _, _ = entry
        return send(
            block(group, origin(way, step), start, size), partner,
            r.pair_send.at[group], r.pair_recv.at[mark(group, way, step)],
        )

    def own_copy(group):
        return send(
            block(group, me, 0, cfg.own[group]), partner, r.pair_send.at[group],
            r.pair_recv.at[mark(group, 1, 0)],
        )

    def landed(ref, sem):
        pltpu.make_async_copy(ref, ref, sem).wait()

    def entries(group, step):
        return [e for e in plan if e[0] == group and e[4] >= step]

    tasks = []

    def own_sends(group, starts=None, last=True):
        for entry in entries(group, 0):
            if starts is None or entry[1] in starts:
                ring_copy(entry, 0).start()
        if last:
            own_copy(group).start()

    def advance(group, step, starts=None):
        for entry in entries(group, step):
            _, start, size, way, far, base = entry
            if starts is not None and start not in starts:
                continue
            landed(block(group, origin(way, step), start, size), r.ring_recv.at[base + step - 1])
            if step < far:
                ring_copy(entry, step).start()
            pair_copy(entry, step).start()
            if tasks:
                tasks.pop(0)()

    def pair_wait(group, way, step):
        slot = origin(way, step) + flip if step else partner
        landed(block(group, slot, 0, cfg.own[group]), r.pair_recv.at[mark(group, way, step)])

    def all_here(group):
        landed(blocks(group, chips), r.pair_recv.at[group])

    def adam_part(ref, part, columns):
        return adam_weights(*(ref[i, part, columns] for i in range(4)))

    upper = cfg.tops[0]

    def adam_qkv(start):
        ready(start, tile_of(start))
        part = pl.ds(pl.multiple_of(me * q_block + start, 16), 16)
        fresh = adam_part(r.q_in, slice(start, start + 16), slice(None))
        r.w_q[part, :] = fresh
        at, lanes = (start, 0) if start < upper else (start - upper, 64)
        r.tails[me, at : at + 16, lanes : lanes + 64] = fresh[:, full:]

    starts = list(range(0, q_block, 16))
    for index, start in enumerate(starts):
        adam_qkv(start)
        if index:
            own_sends(0, starts[index - 1 : index], False)
    ready("o", r.o_in)
    first = pl.multiple_of(me * o_block, 16)
    for part, (start, size) in zip(r.o_part, cfg.segments):
        fresh = adam_part(r.o_in, slice(None), slice(start, start + size))
        part[pl.ds(first, o_block), :] = fresh
    lower = o_block // 2
    r.tails[me, upper:, :64] = fresh[:lower, size - 64 :]
    r.tails[me, upper:, 64:] = fresh[lower:, size - 64 :]
    own_sends(0, starts[-1:])
    own_sends(1)
    ready("tok", r.tok_t)
    for start in range(0, width, 128):
        part = r.tok_t[start : min(start + 128, width), :].astype(f32)
        r.tok[:, start : min(start + 128, width)] = jnp.transpose(part).astype(bf16)
    ready(-1, gain)
    values = r.tok[...].astype(f32)
    mean_sq = jnp.mean(values * values, axis=-1, keepdims=True)
    r.normed[...] = (
        values * lax.rsqrt(mean_sq + norm_eps) * gain[...][None, :]
    ).astype(bf16)
    for index, ref in enumerate(r.small[1:]):
        ready(-2 - index, ref)
    row = lax.broadcasted_iota(jnp.int32, (rows, rows), 0)
    col = lax.broadcasted_iota(jnp.int32, (rows, rows), 1)
    offset = row - col
    across_row = seg_row[...].astype(f32)
    down = jnp.transpose(jnp.broadcast_to(across_row, (128, rows)))
    down = jnp.concatenate([down] * (rows // 128), axis=1)
    allowed = (down == across_row) & (offset >= 0) & (offset < WINDOW)
    r.mask[...] = jnp.where(allowed, 1.0, 0.0)

    def project(start):
        size = min(256, r.w_q.shape[0] - start)
        r.proj[:, start : start + size] = lax.dot_general(
            r.normed[...], r.w_q[start : start + size, :], (((1,), (1,)), ((), ())),
            preferred_element_type=f32,
        )

    lane = lax.broadcasted_iota(jnp.int32, (rows, 128), 1)
    low = lane < HEAD_DIM
    q_rows = cfg.heads * HEAD_DIM
    kv_rows = cfg.kv_heads * HEAD_DIM
    repeat = cfg.heads // cfg.kv_heads
    kept = {}

    def attend(slab):
        allowed = r.mask[...] > 0.0
        zero = jnp.zeros((rows, 128), f32)
        group = slab * 2 // repeat
        if group not in kept:
            base = q_rows + group // 2 * 128
            keys = r.proj[:, base : base + 128]
            keys = keys * cosine[...] + swap_halves(keys, lane) * sine[...]
            vals = r.proj[:, base + kv_rows : base + kv_rows + 128]
            keys_turned, vals_turned = pltpu.roll(keys, HEAD_DIM, 1), pltpu.roll(vals, HEAD_DIM, 1)
            if group % 2 == 1:
                keys, keys_turned, vals, vals_turned = keys_turned, keys, vals_turned, vals
            kept[group] = (
                (jnp.where(low, keys, zero).astype(bf16), jnp.where(low, vals, zero).astype(bf16)),
                (
                    jnp.where(low, zero, keys_turned).astype(bf16),
                    jnp.where(low, zero, vals_turned).astype(bf16),
                ),
            )
        query = r.proj[:, slab * 128 : slab * 128 + 128]
        query = (query * cosine[...] + swap_halves(query, lane) * sine[...]).astype(bf16)
        total = None
        for which, (key_side, val_side) in enumerate(kept[group]):
            scores = lax.dot_general(
                query, key_side, (((1,), (1,)), ((), ())), preferred_element_type=f32
            ) * (HEAD_DIM**-0.5)
            weights = jnp.where(allowed, jnp.exp(scores), 0.0)
            sink = jnp.exp(jnp.full((rows, 1), sinks[2 * slab + which]))
            running = sink + jnp.sum(weights, axis=-1, keepdims=True)
            probs = (weights * (1.0 / running)).astype(bf16)
            part = jnp.dot(probs, val_side, preferred_element_type=f32)
            total = part if total is None else total + part
        r.att[:, slab * 128 : slab * 128 + 128] = total.astype(bf16)

    ours = pl.ds(pl.multiple_of(side * half, half), half)
    theirs = pl.ds(pl.multiple_of(across * half, half), half)

    def swap_copy(index):
        return pltpu.make_async_remote_copy(
            src_ref=r.swap_out[index], dst_ref=r.swap_in[index],
            send_sem=r.swap_send.at[index], recv_sem=r.swap_recv.at[index],
            device_id={"dp": across}, device_id_type=MESH,
        )

    def product(index, which):
        start, size = cfg.segments[index]
        for at in range(0, size, 512):
            span = min(512, size - at)
            part = jnp.dot(
                r.att[ours if which else theirs, :], r.o_part[index][:, at : at + span],
                preferred_element_type=f32,
            )
            if which:
                total = r.tok[ours, start + at : start + at + span].astype(f32) + part
                r.res[:, start + at : start + at + span] = total
            else:
                r.swap_out[index][:, at : at + span] = part.astype(bf16)

    def swap(index):
        product(index, 0)
        swap_copy(index).start()
        product(index, 1)

    def receive(index):
        start, size = cfg.segments[index]
        landed(r.swap_in[index], r.swap_recv.at[index])
        r.res[:, start : start + size] += r.swap_in[index][...].astype(f32)

    heads_slabs = cfg.heads // 2
    spans = range(0, r.w_q.shape[0], 256)

    def unpack_tails():
        part = r.o_part[-1]
        edge = part.shape[1] - 64
        for slot in range(2 * chips):
            low_half, high_half = slice(0, 64), slice(64, 128)
            at = slot * q_block
            r.w_q[at : at + upper, full:] = r.tails[slot, :upper, low_half]
            r.w_q[at + upper : at + q_block, full:] = r.tails[slot, : q_block - upper, high_half]
            at = slot * o_block
            part[at : at + lower, edge:] = r.tails[slot, upper:, low_half]
            part[at + lower : at + o_block, edge:] = r.tails[slot, upper:, high_half]

    advance(0, 1)
    advance(1, 1)
    own_sends(2)
    for step in range(2, hops):
        advance(0, step)
        advance(1, step)
        advance(2, step - 1)
    own_sends(3)
    advance(0, hops)
    advance(1, hops)
    all_here(0)
    all_here(1)
    unpack_tails()
    for start in spans[:3]:
        project(start)
    advance(2, hops - 1)
    own_sends(4)
    for start in spans[3:]:
        project(start)
    for slab in range(heads_slabs // 2):
        attend(slab)
    advance(3, 1)
    for slab in range(heads_slabs // 2, heads_slabs):
        attend(slab)
    advance(2, hops)
    all_here(2)
    swap(0)
    advance(4, 1)
    advance(3, 2)
    advance(4, 2)
    advance(3, 3)
    receive(0)
    r.rows_a[me] = r.res[:, :cut].astype(bf16)
    early, late = (0, half // 4), (half // 2, 3 * half // 4)
    own_sends(fast, early, False)
    advance(4, 3)
    own_sends(fast, late)
    advance(3, 4)
    all_here(3)
    swap(1)
    advance(fast, 1, early)
    advance(4, 4)
    all_here(4)
    swap(2)
    advance(fast, 1, late)
    receive(1)
    advance(fast, 2)
    receive(2)

    experts = router.shape[0]
    top_count = cfg.top_count
    residual = r.res[...]
    mean_sq = jnp.mean(residual * residual, axis=-1, keepdims=True)
    scale = lax.rsqrt(mean_sq + norm_eps)
    head = (r.res[:, :cut] * scale * mlp[:cut][None, :]).astype(bf16)
    tail = (r.res[:, cut:] * scale * mlp[cut:][None, :]).astype(bf16)
    r.rows_b[me] = tail
    edge = tail.shape[1] - 64
    quiet = r.notes.shape[1] - half // 2
    r.notes[me, quiet:, :64] = tail[: half // 2, edge:]
    r.notes[me, quiet:, 64:] = tail[half // 2 :, edge:]
    across_lanes = (((1,), (1,)), ((), ()))
    logits = (
        lax.dot_general(router[:, :cut], head, across_lanes, preferred_element_type=f32)
        + lax.dot_general(router[:, cut:], tail, across_lanes, preferred_element_type=f32)
        + jnp.transpose(jnp.broadcast_to(bias[...], (half, experts)))
    )
    ids = ids_ref[:, ours]
    expert = lax.broadcasted_iota(jnp.int32, (experts, half), 0)
    picked = [ids[k : k + 1, :] == expert for k in range(top_count)]
    hit = sum(jnp.where(p, 1.0, 0.0) for p in picked)
    earlier = lax.broadcasted_iota(jnp.int32, (half, half), 0) < lax.broadcasted_iota(
        jnp.int32, (half, half), 1
    )
    before = jnp.dot(
        hit.astype(bf16), jnp.where(earlier, 1.0, 0.0).astype(bf16), preferred_element_type=f32
    )
    raised = [jnp.exp(jnp.sum(jnp.where(p, logits, 0.0), axis=0, keepdims=True)) for p in picked]
    share = 1.0 / sum(raised)
    line = lax.broadcasted_iota(jnp.int32, (quiet, half), 0)
    note = jnp.zeros(line.shape, f32)
    for k in range(top_count):
        slot = jnp.sum(jnp.where(picked[k], before, 0.0), axis=0, keepdims=True)
        note = jnp.where(line == k, raised[k] * share, note)
        note = jnp.where(line == top_count + k, ids[k : k + 1, :].astype(f32), note)
        note = jnp.where(line == 2 * top_count + k, slot, note)
    rest = jnp.transpose(jnp.broadcast_to(scale, (half, 128)))[:1, :]
    for k in range(3):
        term = rest.astype(bf16).astype(f32)
        note = jnp.where(line == 3 * top_count + k, term, note)
        rest = rest - term
    r.notes[me, :quiet] = note.astype(bf16)

    def take(slot):
        own_expert = me.astype(f32)
        note = r.notes[slot, :quiet].astype(f32)
        r.rows_b[slot, : half // 2, edge:] = r.notes[slot, quiet:, :64]
        r.rows_b[slot, half // 2 :, edge:] = r.notes[slot, quiet:, 64:]
        gate = jnp.zeros((1, half), f32)
        where_to = jnp.full((1, half), -1.0, f32)
        for k in range(top_count):
            chosen = note[top_count + k : top_count + k + 1, :] == own_expert
            gate = jnp.where(chosen, note[k : k + 1, :], gate)
            where_to = jnp.where(chosen, note[2 * top_count + k : 2 * top_count + k + 1, :], where_to)
        at = 3 * top_count
        scales = note[at : at + 1, :] + note[at + 1 : at + 2, :] + note[at + 2 : at + 3, :]
        match = lax.broadcasted_iota(jnp.int32, (capacity, half), 0).astype(f32) == where_to
        select = jnp.where(match, 1.0, 0.0).astype(bf16)
        gates = lax.dot_general(
            jnp.broadcast_to(gate, (8, half)).astype(bf16), select, across_lanes,
            preferred_element_type=f32,
        )
        r.gate_rows[slot] = gates[:1, :]
        scales = jnp.sum(jnp.where(match, scales, 0.0), axis=1, keepdims=True)
        r.out[slot, :, cut:] = jnp.dot(
            select, r.rows_b[slot], preferred_element_type=f32
        ).astype(bf16)
        r.out[slot, :, :cut] = (
            jnp.dot(select, r.rows_a[slot], preferred_element_type=f32)
            * scales * mlp[:cut][None, :]
        ).astype(bf16)

    own_sends(marks)
    own_sends(slow)
    advance(fast, 3)
    take(me)

    def ring_task(way, step):
        return lambda: take(origin(way, step))

    def pair_task(ways, step):
        def run():
            for group in (fast, slow, marks):
                pair_wait(group, ways[0], step)
            take(origin(ways[0], step) + flip)
        return run

    def partner_task():
        for group in (fast, slow, marks):
            pair_wait(group, 1, 0)
        take(partner)

    tasks.append(partner_task)
    for step in range(1, hops + 1):
        advance(marks, step)
        advance(slow, step)
        if step == 1:
            advance(fast, 4)
        for ways in ((1,), (-1,)) if step < hops else ((1, -1),):
            tasks.append(ring_task(ways[0], step))
            tasks.append(pair_task(ways, step))
    while tasks:
        tasks.pop(0)()
    r.gates[...] = r.gate_rows[:, 0, :].astype(bf16)

    for group in range(marks + 1):
        landed(blocks(group, chips - 1), r.ring_send.at[group])
        landed(blocks(group, chips), r.pair_send.at[group])
    for index in range(swaps):
        swap_copy(index).wait_send()


def layer_call(
    tokens, segments, expert_ids, gain, sinks, adam, router_weight, router_bias, mlp_gain,
    heads, kv_heads, sources, experts, capacity,
):
    rows, width = tokens.shape
    half = rows // 2
    chips = sources // 2
    hops = chips // 2
    q_block, o_block = adam[0].shape[0], adam[4].shape[0]
    top_count = expert_ids.shape[1]
    cut = width * 3 // 8 // 128 * 128
    segments_o = ((0, cut), (cut, cut), (2 * cut, width - 2 * cut))
    tiles = q_block // 16
    q_spans = [(16 * t, 16, 1 if t < (tiles + 1) // 2 else -1) for t in range(tiles)]
    o_spans = [(0, o_block // 2, 1), (o_block // 2, o_block // 2, -1)]
    last_spans = [(0, 16, 1), (16, o_block - 16, -1)]
    quarter = half // 4
    r_spans = [(quarter * t, quarter, 1 if t < 2 else -1) for t in range(4)]
    tops = (q_block + 31) // 32 * 16, o_block // 2
    tail_rows, note_rows = sum(tops), 16 + half // 2

    def two_spans(count):
        first = (count + 31) // 32 * 16
        return [(0, first, 1), (first, count - first, -1)]

    spans = (
        q_spans, two_spans(tail_rows), o_spans, o_spans, last_spans, r_spans, r_spans,
        two_spans(note_rows),
    )
    plan, total = piece_plan(spans, hops)
    cosine, sine = split_tables(rows)
    bf16, f32 = jnp.bfloat16, jnp.float32
    hbm = dict(
        tok=tokens.T, adam=adam,
        small=[
            gain, mlp_gain, segments[None, :], jnp.asarray(cosine), jnp.asarray(sine),
            router_weight.T, router_bias[None, :], expert_ids.T, sinks,
        ],
    )
    small = [pltpu.VMEM(v.shape, v.dtype) for v in hbm["small"][:-1]]
    dma = pltpu.SemaphoreType.DMA
    groups, swaps = len(spans), len(segments_o)
    scratch = dict(
        tok=pltpu.VMEM(tokens.shape, bf16),
        tok_t=pltpu.VMEM((width, rows), bf16),
        small=small + [pltpu.SMEM(sinks.shape, sinks.dtype)],
        mask=pltpu.VMEM((rows, rows), f32),
        q_in=pltpu.VMEM((4, q_block, width), f32),
        o_in=pltpu.VMEM((4, o_block, width), f32),
        normed=pltpu.VMEM((rows, width), bf16),
        w_q=pltpu.VMEM((sources * q_block, width), bf16),
        tails=pltpu.VMEM((sources, tail_rows, 128), bf16),
        o_part=[pltpu.VMEM((sources * o_block, size), bf16) for _, size in segments_o],
        proj=pltpu.VMEM((rows, sources * q_block), f32),
        att=pltpu.VMEM((rows, heads * HEAD_DIM), bf16),
        res=pltpu.VMEM((half, width), f32),
        swap_out=[pltpu.VMEM((half, size), bf16) for _, size in segments_o],
        swap_in=[pltpu.VMEM((half, size), bf16) for _, size in segments_o],
        rows_a=pltpu.VMEM((sources, half, cut), bf16),
        rows_b=pltpu.VMEM((sources, half, width - cut), bf16),
        notes=pltpu.VMEM((sources, note_rows, half), bf16),
        gate_rows=pltpu.VMEM((sources, 1, capacity), f32),
        load_sem=dma((tiles + 11,)),
        ring_send=dma((groups,)),
        ring_recv=dma((total,)),
        pair_send=dma((groups,)),
        pair_recv=dma((groups - 3 + 3 * chips,)),
        swap_send=dma((swaps,)),
        swap_recv=dma((swaps,)),
    )
    results = dict(
        out=pltpu.VMEM((sources, capacity, width), bf16),
        gates=pltpu.VMEM((sources, capacity), bf16),
    )
    operands, hbm_tree = jax.tree.flatten(hbm)
    outputs, result_tree = jax.tree.flatten(results)
    buffers, scratch_tree = jax.tree.flatten(scratch)
    own = (q_block, tail_rows, *[o_block] * swaps, half, half, note_rows)
    cfg = types.SimpleNamespace(
        plan=plan, own=own, chips=chips, heads=heads, kv_heads=kv_heads, segments=segments_o,
        top_count=top_count, tops=tops,
    )

    def body(*refs):
        taken = list(refs)
        spaces = []
        for tree in (hbm_tree, result_tree, scratch_tree):
            count = tree.num_leaves
            spaces.append(jax.tree.unflatten(tree, taken[:count]))
            taken = taken[count:]
        layer_kernel(
            cfg, types.SimpleNamespace(**spaces[0]),
            types.SimpleNamespace(**spaces[1], **spaces[2]),
        )

    gates, out = pl.pallas_call(
        body,
        out_shape=outputs,
        in_specs=[pl.BlockSpec(memory_space=pltpu.HBM)] * len(operands),
        out_specs=[pl.BlockSpec(memory_space=pltpu.VMEM)] * 2,
        scratch_shapes=buffers,
        compiler_params=pltpu.CompilerParams(
            collective_id=4, has_side_effects=True, vmem_limit_bytes=48 * 1024 * 1024
        ),
        name="layer",
    )(*(pltpu.with_memory_space_constraint(v, pltpu.HBM) for v in operands))
    return out, gates


def layer_fits(tokens, adam, sources, experts, capacity, groups):
    rows, width = tokens.shape
    return (
        groups == 2 and experts == sources and sources == 16 and rows == 256
        and adam[0].shape[0] % 16 == 0 and adam[4].shape[0] % 32 == 0
        and width % 128 == 64 and width >= 1024 and capacity <= 128
    )


def on_device(
    tokens,
    segment_ids,
    expert_ids,
    attn_gain,
    sinks,
    qkv_master,
    qkv_mom,
    qkv_var,
    qkv_grad,
    o_master,
    o_mom,
    o_var,
    o_grad,
    router_weight,
    router_bias,
    mlp_gain,
):
    tok_rows, width = tokens.shape
    half = tok_rows // lax.axis_size("dp")
    sources = lax.axis_size("expert")
    heads_here = sinks.shape[0]
    kv_here = KV_HEADS * heads_here // HEADS
    experts = router_weight.shape[1]
    top_count = expert_ids.shape[1]
    capacity = 2 * half * top_count // experts
    adam = [qkv_master, qkv_mom, qkv_var, qkv_grad, o_master, o_mom, o_var, o_grad]
    if layer_fits(tokens, adam, sources, experts, capacity, lax.axis_size("dp")):
        dispatched, gate_slots = layer_call(
            tokens, segment_ids, expert_ids, attn_gain, sinks, adam, router_weight, router_bias,
            mlp_gain, heads_here, kv_here, sources, experts, capacity,
        )
        return (dispatched[None, :, None], gate_slots[None, :, None])
    qkv_local = adam_weights(qkv_master, qkv_mom, qkv_var, qkv_grad)
    o_local = adam_weights(o_master, o_mom, o_var, o_grad)
    qkv_full, o_full = gather_rows([qkv_local, o_local], sources, 1)
    part = attention_call(
        tokens, attn_gain, qkv_full, o_full, segment_ids, sinks, heads_here, kv_here
    ).reshape(-1, half, width)
    got = exchange_call(part, 2)
    rows = router_call(
        tokens, part, got, mlp_gain, router_weight, router_bias, expert_ids, 128 - width % 128
    )
    compact = sources * half <= 2 * experts * capacity
    if experts == sources and compact and ring_fits([rows], sources):
        dispatched, gate_slots = ring_gather(
            [rows], 4, sources, 3, (top_count, capacity, width)
        )
        return (dispatched[None, :, None], gate_slots[None])
    return exchange_slots(rows, width, experts, capacity, top_count, sources)


def solution(mesh):
    return jax.shard_map(
        on_device,
        mesh=mesh,
        in_specs=(
            P("expert", None),
            P("expert"),
            P("expert", None),
            P(),
            P("dp"),
            P(("dp", "expert"), None),
            P(("dp", "expert"), None),
            P(("dp", "expert"), None),
            P(("dp", "expert"), None),
            P(("dp", "expert"), None),
            P(("dp", "expert"), None),
            P(("dp", "expert"), None),
            P(("dp", "expert"), None),
            P(),
            P(),
            P(),
        ),
        out_specs=(P("expert", None, "dp", None, None), P("expert", None, "dp", None)),
        check_vma=False,
    )
```

```python
import functools
import types

import jax
import jax.numpy as jnp
import numpy as np
from jax import lax
from jax.experimental import pallas as pl
from jax.experimental.pallas import tpu as pltpu
from jax.sharding import PartitionSpec as P

HEADS = 32
KV_HEADS = 4
HEAD_DIM = 64
WINDOW = 128
MESH = pl.DeviceIdType.MESH
VMEM_BYTES = 36 * 1024 * 1024


beta_one = 0.9
beta_two = 0.999
adam_step = 100
learn_rate = 0.02
adam_eps = 1e-08
norm_eps = 1e-05
rope_base = 150000.0


def adam_weights(master, moment, second_mom, gradient):
    moment_new = beta_one * moment + (1.0 - beta_one) * gradient
    second_new = beta_two * second_mom + (1.0 - beta_two) * gradient * gradient
    fix_one = 1.0 - beta_one**adam_step
    fix_two = 1.0 - beta_two**adam_step
    update = moment_new / fix_one / (jnp.sqrt(second_new / fix_two) + adam_eps)
    return (master - learn_rate * update).astype(jnp.bfloat16)


def rotation_tables(rows):
    half_dim = HEAD_DIM // 2
    positions = jnp.arange(rows).astype(jnp.float32)
    frequency = rope_base ** (-(jnp.arange(half_dim).astype(jnp.float32) * 2.0) / HEAD_DIM)
    angles = positions[:, None] * frequency[None, :]
    cosine = jnp.cos(angles)
    sine = jnp.sin(angles)
    return (
        jnp.concatenate([cosine] * 4, axis=1),
        jnp.concatenate([-sine, sine, -sine, sine], axis=1),
    )


def chip_at(place, chips):
    place = lax.rem(place + 2 * chips, chips)
    return jnp.where(place < chips // 2, 2 * place, 2 * (chips - 1 - place) + 1)


def gather_kernel(chips, plan, top_count, *refs):
    count = len({entry[0] for entry in plan})
    if top_count:
        (source, out_ref, gate_ref, held), sems = refs[:4], refs[4:]
        ins, outs = (source,), (held,)
    else:
        ins, outs, sems = refs[:count], refs[count : 2 * count], refs[2 * count :]
    ring_send, ring_recv, pair_send, pair_recv, own_send, own_recv, own_sem = sems
    me = lax.axis_index("expert")
    core = lax.rem(me, 2)
    chip = me // 2
    place = jnp.where(lax.rem(chip, 2) == 0, chip // 2, chips - 1 - chip // 2)
    right = chip_at(place + 1, chips) * 2 + core
    left = chip_at(place - 1, chips) * 2 + core
    partner = me + 1 - 2 * core

    barrier = pltpu.get_barrier_semaphore()
    for other in (left, right, partner):
        pl.semaphore_signal(barrier, inc=1, device_id={"expert": other}, device_id_type=MESH)
    pl.semaphore_wait(barrier, 3)

    def block(j, slot):
        arr, start, size = plan[j][:3]
        return outs[arr].at[slot, pl.ds(start, size)]

    def origin(way, step):
        return chip_at(place - step if way > 0 else place + step, chips) * 2 + core

    def copy_to(j, step, send, recv, target):
        arr, start, size, way, _ = plan[j]
        slot = origin(way, step)
        return pltpu.make_async_remote_copy(
            src_ref=ins[arr].at[pl.ds(start, size)] if step == 0 else block(j, slot),
            dst_ref=block(j, slot),
            send_sem=send.at[j, step],
            recv_sem=recv.at[j, step],
            device_id={"expert": target},
            device_id_type=MESH,
        )

    def ring_copy(j, step):
        return copy_to(j, step, ring_send, ring_recv, right if plan[j][3] > 0 else left)

    def pair_copy(j, step):
        return copy_to(j, step, pair_send, pair_recv, partner)

    def own_copy(arr, slot):
        return pltpu.make_async_remote_copy(
            src_ref=ins[arr],
            dst_ref=outs[arr].at[slot],
            send_sem=own_send.at[arr],
            recv_sem=own_recv.at[arr],
            device_id={"expert": partner},
            device_id_type=MESH,
        )

    def landed(j, slot, sem):
        pltpu.make_async_copy(block(j, slot), block(j, slot), sem).wait()

    def consume(rows, slot):
        if top_count:
            fill_slots(top_count, rows, out_ref, gate_ref, slot)

    def take_mine():
        consume(ins[0], me)

    def take_partner():
        for arr in range(count):
            pltpu.make_async_copy(
                outs[arr].at[partner], outs[arr].at[partner], own_recv.at[arr]
            ).wait()
        consume(outs[0].at[partner], partner)

    def take_ring(way, step):
        slot = origin(way, step)
        consume(outs[0].at[slot], slot)

    def take_pair(ways, step):
        for j, entry in enumerate(plan):
            if entry[3] in ways and step <= entry[4]:
                landed(j, origin(entry[3], step) + 1 - 2 * core, pair_recv.at[j, step])
        slot = origin(ways[0], step) + 1 - 2 * core
        consume(outs[0].at[slot], slot)

    every = range(len(plan))
    hops = chips // 2
    for j in every:
        ring_copy(j, 0).start()
    for arr in range(count):
        own_copy(arr, me).start()
    owns = []
    if not top_count:
        owns = [
            pltpu.make_async_copy(ins[a], outs[a].at[me], own_sem.at[a]) for a in range(count)
        ]
    for copy in owns:
        copy.start()
    tasks = [take_mine, take_partner]
    for step in range(1, hops + 1):
        for j in every:
            if step > plan[j][4]:
                continue
            landed(j, origin(plan[j][3], step), ring_recv.at[j, step - 1])
            if step < plan[j][4]:
                ring_copy(j, step).start()
            pair_copy(j, step).start()
            if tasks:
                tasks.pop(0)()
        for ways in ((1,), (-1,)) if step < hops else ((1, -1),):
            tasks.append(functools.partial(take_ring, ways[0], step))
            tasks.append(functools.partial(take_pair, ways, step))
    tasks = tasks[::2] + tasks[1::2]
    for task in tasks:
        task()
    for copy in owns:
        copy.wait()
    for arr in range(count):
        own_copy(arr, me).wait_send()
    for j in every:
        for step in range(plan[j][4] + 1):
            if step:
                pair_copy(j, step).wait_send()
            if step < plan[j][4]:
                ring_copy(j, step).wait_send()


def ring_gather(arrays, cuts, sources, call_id, slots=None):
    plan = []
    chips = sources // 2
    for arr, value in enumerate(arrays):
        tiles = value.shape[0] // 16
        for cut in range(cuts):
            start = (tiles * cut + cuts - 1) // cuts * 16
            size = (tiles * (cut + 1) + cuts - 1) // cuts * 16 - start
            for way in (1, -1):
                far = (cut < cuts // 2) == (way > 0)
                plan.append((arr, start, size, way, chips // 2 - (0 if far else 1)))
    copies, count = len(plan), len(arrays)
    gathered = [jax.ShapeDtypeStruct((sources, *v.shape), v.dtype) for v in arrays]
    sems = [pltpu.SemaphoreType.DMA((copies, chips // 2 + 1))] * 4
    sems += [pltpu.SemaphoreType.DMA((count,))] * 3
    vmem = pl.BlockSpec(memory_space=pltpu.VMEM)
    if slots:
        top_count, capacity, width = slots
        out_shape = (
            jax.ShapeDtypeStruct((sources, capacity, width), jnp.bfloat16),
            jax.ShapeDtypeStruct((sources, 1, capacity), jnp.bfloat16),
        )
        out_specs = (vmem, vmem)
        held = [pltpu.VMEM(gathered[0].shape, gathered[0].dtype)]
    else:
        top_count, out_shape, held = 0, gathered, []
        out_specs = [vmem] * count
    return pl.pallas_call(
        functools.partial(gather_kernel, chips, tuple(plan), top_count),
        out_shape=out_shape,
        in_specs=[vmem] * count,
        out_specs=out_specs,
        scratch_shapes=held + sems,
        compiler_params=pltpu.CompilerParams(
            collective_id=call_id, has_side_effects=True,
            vmem_limit_bytes=(40 if slots else 24) * 1024 * 1024,
        ),
        name="ring_slots" if slots else "ring_gather",
    )(*arrays)


def ring_fits(arrays, sources):
    return sources % 4 == 0 and 8 <= sources <= 32 and all(a.shape[0] % 16 == 0 for a in arrays)


def gather_rows(arrays, sources, call_id):
    if ring_fits(arrays, sources):
        width = arrays[0].shape[1]
        return [v.reshape(-1, width) for v in ring_gather(arrays, 2, sources, call_id)]
    return [lax.all_gather(a, "expert", axis=0, tiled=True) for a in arrays]


def swap_halves(values, lane):
    up = pltpu.roll(values, 128 - HEAD_DIM // 2, 1)
    down = pltpu.roll(values, HEAD_DIM // 2, 1)
    return jnp.where(lane % HEAD_DIM < HEAD_DIM // 2, up, down)


def attention_kernel(
    heads, kv_heads, tok_ref, gain_ref, w_ref, o_ref, cos_ref, sin_ref, seg_col, seg_row, sink_ref,
    out_ref, proj_ref, att_ref,
):
    rows = tok_ref.shape[0]
    bf16 = jnp.bfloat16
    values = tok_ref[...].astype(jnp.float32)
    mean_sq = jnp.mean(values * values, axis=-1, keepdims=True)
    normed = (values * lax.rsqrt(mean_sq + norm_eps) * gain_ref[...][None, :]).astype(bf16)
    features = w_ref.shape[0]
    for start in range(0, features, 256):
        size = min(256, features - start)
        proj_ref[:, start : start + size] = lax.dot_general(
            normed, w_ref[start : start + size, :], (((1,), (1,)), ((), ())),
            preferred_element_type=jnp.float32,
        )
    lane = lax.broadcasted_iota(jnp.int32, (rows, 128), 1)
    low = lane < HEAD_DIM
    cosine, sine = cos_ref[...], sin_ref[...]
    row = lax.broadcasted_iota(jnp.int32, (rows, rows), 0)
    col = lax.broadcasted_iota(jnp.int32, (rows, rows), 1)
    offset = row - col
    allowed = (seg_col[...] == seg_row[...]) & (offset >= 0) & (offset < WINDOW)
    q_rows = heads * HEAD_DIM
    kv_rows = kv_heads * HEAD_DIM
    repeat = heads // kv_heads
    zero = jnp.zeros((rows, 128), jnp.float32)
    for group in range(kv_heads):
        base = q_rows + group // 2 * 128
        keys = proj_ref[:, base : base + 128]
        keys = keys * cosine + swap_halves(keys, lane) * sine
        vals = proj_ref[:, base + kv_rows : base + kv_rows + 128]
        keys_turned, vals_turned = pltpu.roll(keys, HEAD_DIM, 1), pltpu.roll(vals, HEAD_DIM, 1)
        if group % 2 == 1:
            keys, keys_turned, vals, vals_turned = keys_turned, keys, vals_turned, vals
        sides = (
            (jnp.where(low, keys, zero).astype(bf16), jnp.where(low, vals, zero).astype(bf16)),
            (
                jnp.where(low, zero, keys_turned).astype(bf16),
                jnp.where(low, zero, vals_turned).astype(bf16),
            ),
        )
        for slab in range(group * repeat // 2, (group + 1) * repeat // 2):
            query = proj_ref[:, slab * 128 : slab * 128 + 128]
            query = (query * cosine + swap_halves(query, lane) * sine).astype(bf16)
            total = None
            for side, (key_side, val_side) in enumerate(sides):
                scores = lax.dot_general(
                    query, key_side, (((1,), (1,)), ((), ())), preferred_element_type=jnp.float32
                ) * (HEAD_DIM**-0.5)
                weights = jnp.where(allowed, jnp.exp(scores), 0.0)
                running = jnp.exp(jnp.full((rows, 1), sink_ref[2 * slab + side])) + jnp.sum(weights, axis=-1, keepdims=True)
                probs = (weights * (1.0 / running)).astype(bf16)
                part = jnp.dot(probs, val_side, preferred_element_type=jnp.float32)
                total = part if total is None else total + part
            att_ref[:, slab * 128 : slab * 128 + 128] = total.astype(bf16)
    width = o_ref.shape[1]
    for start in range(0, width, 384):
        size = min(384, width - start)
        out_ref[:, start : start + size] = jnp.dot(
            att_ref[...], o_ref[:, start : start + size], preferred_element_type=jnp.float32
        ).astype(bf16)


def attention_call(tokens, gain, qkv_full, o_full, segments, sinks, heads, kv_heads):
    rows, width = tokens.shape
    cosine, sine = rotation_tables(rows)
    vmem = pl.BlockSpec(memory_space=pltpu.VMEM)
    return pl.pallas_call(
        functools.partial(attention_kernel, heads, kv_heads),
        out_shape=jax.ShapeDtypeStruct((rows, width), jnp.bfloat16),
        in_specs=[vmem] * 8 + [pl.BlockSpec(memory_space=pltpu.SMEM)],
        out_specs=vmem,
        scratch_shapes=[
            pltpu.VMEM((rows, qkv_full.shape[0]), jnp.float32),
            pltpu.VMEM((rows, heads * HEAD_DIM), jnp.bfloat16),
        ],
        compiler_params=pltpu.CompilerParams(vmem_limit_bytes=VMEM_BYTES),
        name="attention_part",
    )(
        tokens, gain, qkv_full, o_full, cosine, sine, segments[:, None],
        segments[None, :], sinks,
    )


def exchange_kernel(part_ref, got_ref, send_sem, recv_sem):
    group = lax.axis_index("dp")
    other = 1 - group
    barrier = pltpu.get_barrier_semaphore()
    pl.semaphore_signal(barrier, inc=1, device_id={"dp": other}, device_id_type=MESH)
    pl.semaphore_wait(barrier, 1)
    copy = pltpu.make_async_remote_copy(
        src_ref=part_ref.at[other],
        dst_ref=got_ref,
        send_sem=send_sem,
        recv_sem=recv_sem,
        device_id={"dp": other},
        device_id_type=MESH,
    )
    copy.start()
    copy.wait()


def exchange_call(part, call_id):
    return pl.pallas_call(
        exchange_kernel,
        out_shape=jax.ShapeDtypeStruct(part.shape[1:], part.dtype),
        in_specs=[pl.BlockSpec(memory_space=pltpu.VMEM)],
        out_specs=pl.BlockSpec(memory_space=pltpu.VMEM),
        scratch_shapes=[pltpu.SemaphoreType.DMA, pltpu.SemaphoreType.DMA],
        compiler_params=pltpu.CompilerParams(
            collective_id=call_id, has_side_effects=True, vmem_limit_bytes=16 * 1024 * 1024
        ),
        name="exchange_halves",
    )(part)


def router_kernel(tok_ref, part_ref, got_ref, gain_ref, rw_ref, bias_ref, ids_ref, out_ref):
    group = lax.axis_index("dp")
    half, width = got_ref.shape
    experts = rw_ref.shape[0]
    top_count = ids_ref.shape[1]
    rows = pl.ds(pl.multiple_of(group * half, half), half)
    summed = part_ref[group].astype(jnp.float32) + got_ref[...].astype(jnp.float32)
    residual = tok_ref[rows, :].astype(jnp.float32) + summed
    mean_sq = jnp.mean(residual * residual, axis=-1, keepdims=True)
    moe_in = (residual * lax.rsqrt(mean_sq + norm_eps) * gain_ref[...][None, :]).astype(jnp.bfloat16)
    out_ref[:, :width] = moe_in
    logits = lax.dot_general(
        moe_in, rw_ref[...], (((1,), (1,)), ((), ())), preferred_element_type=jnp.float32
    ) + bias_ref[...]
    ids = ids_ref[rows, :]
    expert = lax.broadcasted_iota(jnp.int32, (half, experts), 1)
    picked = [ids[:, k : k + 1] == expert for k in range(top_count)]
    hit = sum(jnp.where(p, 1.0, 0.0) for p in picked)
    above = lax.broadcasted_iota(jnp.int32, (half, half), 0) > lax.broadcasted_iota(
        jnp.int32, (half, half), 1
    )
    before = jnp.dot(
        jnp.where(above, 1.0, 0.0).astype(jnp.bfloat16), hit.astype(jnp.bfloat16),
        preferred_element_type=jnp.float32,
    )
    raised = [jnp.exp(jnp.sum(jnp.where(p, logits, 0.0), axis=1, keepdims=True)) for p in picked]
    scale = 1.0 / sum(raised)
    column = lax.broadcasted_iota(jnp.int32, (half, out_ref.shape[1] - width), 1)
    extra = jnp.zeros(column.shape, jnp.float32)
    for k in range(top_count):
        slot = jnp.sum(jnp.where(picked[k], before, 0.0), axis=1, keepdims=True)
        extra = jnp.where(column == 3 * k, raised[k] * scale, extra)
        extra = jnp.where(column == 3 * k + 1, ids[:, k : k + 1].astype(jnp.float32), extra)
        extra = jnp.where(column == 3 * k + 2, slot, extra)
    out_ref[:, width:] = extra.astype(jnp.bfloat16)


def router_call(tokens, part, got, gain, router_weight, router_bias, expert_ids, extra):
    half, width = got.shape
    return pl.pallas_call(
        router_kernel,
        out_shape=jax.ShapeDtypeStruct((half, width + extra), jnp.bfloat16),
        in_specs=[pl.BlockSpec(memory_space=pltpu.VMEM)] * 7,
        out_specs=pl.BlockSpec(memory_space=pltpu.VMEM),
        compiler_params=pltpu.CompilerParams(vmem_limit_bytes=VMEM_BYTES),
        name="router_part",
    )(tokens, part, got, gain, router_weight.T, router_bias[None, :], expert_ids)


def fill_slots(top_count, rows_ref, out_ref, gate_ref, slot):
    mine = lax.axis_index("expert").astype(jnp.float32)
    _, capacity, width = out_ref.shape
    half, full = rows_ref.shape
    extra = rows_ref[:, full - 128 :].astype(jnp.float32)
    shift = 128 - (full - width)
    place = lax.broadcasted_iota(jnp.int32, (half, capacity), 1).astype(jnp.float32)
    select = jnp.zeros((half, capacity), jnp.float32)
    gates = jnp.zeros((half, capacity), jnp.float32)
    for k in range(top_count):
        at = shift + 3 * k
        match = (extra[:, at + 1 : at + 2] == mine) & (extra[:, at + 2 : at + 3] == place)
        select = jnp.where(match, 1.0, select)
        gates = jnp.where(match, extra[:, at : at + 1], gates)
    gate_ref[slot] = jnp.sum(gates, axis=0, keepdims=True).astype(jnp.bfloat16)
    out_ref[slot] = lax.dot_general(
        select.astype(jnp.bfloat16), rows_ref[:, :width], (((0,), (0,)), ((), ())),
        preferred_element_type=jnp.float32,
    ).astype(jnp.bfloat16)


def exchange_slots(rows, width, experts, capacity, top_count, sources):
    half = rows.shape[0]
    extra = rows[:, width:].astype(jnp.float32)
    moe_in = rows[:, :width]
    gates, ids, slots = (extra[:, i : 3 * top_count : 3] for i in range(3))
    target = (ids * capacity + slots).astype(jnp.int32).reshape(-1)
    matches = target[None, :] == jnp.arange(experts * capacity, dtype=jnp.int32)[:, None]
    token_match = jnp.any(matches.reshape(experts * capacity, half, top_count), axis=2)
    payload = jnp.dot(
        token_match.astype(jnp.bfloat16), moe_in, preferred_element_type=jnp.float32
    ).astype(jnp.bfloat16)
    slot_gates = jnp.sum(jnp.where(matches, gates.reshape(-1)[None, :], 0.0), axis=1)
    outgoing = (
        payload.reshape(experts, capacity, width),
        slot_gates.astype(jnp.bfloat16).reshape(experts, capacity),
    )
    got_rows, got_gates = (
        lax.all_to_all(v, "expert", split_axis=0, concat_axis=0, tiled=True) for v in outgoing
    )
    per_device = experts // sources
    got_rows = got_rows.reshape(sources, per_device, capacity, width)
    got_gates = got_gates.reshape(sources, per_device, capacity)
    return (
        jnp.transpose(got_rows, (1, 0, 2, 3))[:, :, None],
        jnp.transpose(got_gates, (1, 0, 2))[:, :, None],
    )


def split_tables(rows):
    half_dim = HEAD_DIM // 2
    positions = np.arange(rows).astype(np.float64)
    powers = -(np.arange(half_dim).astype(np.float64) * 2.0) / HEAD_DIM
    frequency = (rope_base**powers).astype(np.float32).astype(np.float64)
    angles = (positions[:, None] * frequency[None, :]).astype(np.float32).astype(np.float64)
    cosine, sine = np.cos(angles), np.sin(angles)
    return (
        np.concatenate([cosine] * 4, axis=1).astype(np.float32),
        np.concatenate([-sine, sine, -sine, sine], axis=1).astype(np.float32),
    )


def piece_plan(groups, hops):
    plan, base = [], 0
    for group, spans in enumerate(groups):
        for start, size, far_way in spans:
            for way in (1, -1):
                count = hops if way == far_way else hops - 1
                plan.append((group, start, size, way, count, base))
                base += count
    return tuple(plan), base


def layer_kernel(cfg, hbm, r):
    bf16, f32 = jnp.bfloat16, jnp.float32
    chips, plan = cfg.chips, cfg.plan
    hops = chips // 2
    me = lax.axis_index("expert")
    side = lax.axis_index("dp")
    core = lax.rem(me, 2)
    chip = me // 2
    place = jnp.where(lax.rem(chip, 2) == 0, chip // 2, chips - 1 - chip // 2)
    right = chip_at(place + 1, chips) * 2 + core
    left = chip_at(place - 1, chips) * 2 + core
    flip = 1 - 2 * core
    partner = me + flip
    across = 1 - side
    rows, width = r.tok.shape
    half = rows // 2
    q_block = r.q_in.shape[1]
    o_block = r.o_in.shape[1]
    capacity = r.out.shape[1]
    cut = cfg.segments[0][1]

    names = []

    def load(name, pairs):
        for src, dst in pairs:
            pltpu.make_async_copy(src, dst, r.load_sem.at[len(names)]).start()
        names.append(name)

    def ready(name, ref):
        pltpu.make_async_copy(ref, ref, r.load_sem.at[names.index(name)]).wait()

    def tile_of(start):
        return r.q_in.at[:, pl.ds(start, 16)]

    for start in range(0, q_block, 16):
        part = pl.ds(start, 16)
        load(start, [(hbm.adam[i].at[part], r.q_in.at[i, part]) for i in range(4)])
    load("tok", [(hbm.tok, r.tok_t)])
    load("o", [(hbm.adam[4 + i], r.o_in.at[i]) for i in range(4)])
    for index, pair in enumerate(zip(hbm.small, r.small)):
        load(-1 - index, [pair])
    gain, mlp, seg_row, cosine, sine, router, bias, ids_ref, sinks = r.small

    barrier = pltpu.get_barrier_semaphore()
    for other in (left, right, partner):
        pl.semaphore_signal(barrier, inc=1, device_id={"expert": other}, device_id_type=MESH)
    pl.semaphore_signal(barrier, inc=1, device_id={"dp": across}, device_id_type=MESH)

    swaps = len(cfg.segments)
    fast, slow, marks = swaps + 2, swaps + 3, swaps + 4
    full = width // 128 * 128
    held = (r.w_q, r.tails, *r.o_part, r.rows_a, r.rows_b, r.notes)
    stride = (q_block, 0, *[o_block] * swaps, 0, 0, 0)

    def block(group, slot, start, size):
        ref = held[group]
        columns = pl.ds(0, ref.shape[-1] // 128 * 128)
        if stride[group]:
            first = pl.multiple_of(slot * stride[group] + start, 16)
            return ref.at[pl.ds(first, size), columns]
        return ref.at[slot, pl.ds(start, size), columns]

    def blocks(group, count):
        if stride[group]:
            return block(group, 0, 0, count * stride[group])
        columns = pl.ds(0, held[group].shape[-1] // 128 * 128)
        return held[group].at[pl.ds(0, count), :, columns]

    def origin(way, step):
        return chip_at(place - step if way > 0 else place + step, chips) * 2 + core

    def send(ref, device, out_sem, in_sem):
        return pltpu.make_async_remote_copy(
            src_ref=ref, dst_ref=ref, send_sem=out_sem, recv_sem=in_sem,
            device_id={"expert": device}, device_id_type=MESH,
        )

    def ring_copy(entry, step):
        group, start, size, way, _, base = entry
        return send(
            block(group, origin(way, step), start, size), right if way > 0 else left,
            r.ring_send.at[group], r.ring_recv.at[base + step],
        )

    def mark(group, way, step):
        if group < fast:
            return group
        at = fast + 2 * hops * (group - fast)
        return at if step == 0 else at + (2 * step - (way > 0) if step < hops else 2 * step - 1)

    def pair_copy(entry, step):
        group, start, size, way, _, _ = entry
        return send(
            block(group, origin(way, step), start, size), partner,
            r.pair_send.at[group], r.pair_recv.at[mark(group, way, step)],
        )

    def own_copy(group):
        return send(
            block(group, me, 0, cfg.own[group]), partner, r.pair_send.at[group],
            r.pair_recv.at[mark(group, 1, 0)],
        )

    def landed(ref, sem):
        pltpu.make_async_copy(ref, ref, sem).wait()

    def entries(group, step):
        return [e for e in plan if e[0] == group and e[4] >= step]

    tasks = []

    def own_sends(group, starts=None, last=True):
        for entry in entries(group, 0):
            if starts is None or entry[1] in starts:
                ring_copy(entry, 0).start()
        if last:
            own_copy(group).start()

    def advance(group, step, starts=None):
        for entry in entries(group, step):
            _, start, size, way, far, base = entry
            if starts is not None and start not in starts:
                continue
            landed(block(group, origin(way, step), start, size), r.ring_recv.at[base + step - 1])
            if step < far:
                ring_copy(entry, step).start()
            pair_copy(entry, step).start()
            if tasks:
                tasks.pop(0)()

    def pair_wait(group, way, step):
        slot = origin(way, step) + flip if step else partner
        landed(block(group, slot, 0, cfg.own[group]), r.pair_recv.at[mark(group, way, step)])

    def all_here(group):
        landed(blocks(group, chips), r.pair_recv.at[group])

    def adam_part(ref, part, columns):
        return adam_weights(*(ref[i, part, columns] for i in range(4)))

    upper = cfg.tops[0]

    def adam_qkv(start):
        ready(start, tile_of(start))
        part = pl.ds(pl.multiple_of(me * q_block + start, 16), 16)
        fresh = adam_part(r.q_in, slice(start, start + 16), slice(None))
        r.w_q[part, :] = fresh
        at, lanes = (start, 0) if start < upper else (start - upper, 64)
        r.tails[me, at : at + 16, lanes : lanes + 64] = fresh[:, full:]

    starts_done = {start + size: (start,) for group, start, size, *_ in plan if group == 0}
    for start in range(0, q_block, 16):
        adam_qkv(start)
        if start == 16:
            pl.semaphore_wait(barrier, 4)
        own_sends(0, starts_done.get(start, ()), False)
    ready("o", r.o_in)
    first = pl.multiple_of(me * o_block, 16)
    for part, (start, size) in zip(r.o_part, cfg.segments):
        fresh = adam_part(r.o_in, slice(None), slice(start, start + size))
        part[pl.ds(first, o_block), :] = fresh
    lower = o_block // 2
    r.tails[me, upper:, :64] = fresh[:lower, size - 64 :]
    r.tails[me, upper:, 64:] = fresh[lower:, size - 64 :]
    own_sends(0, starts_done[q_block])
    own_sends(1)
    ready("tok", r.tok_t)
    for start in range(0, width, 128):
        part = r.tok_t[start : min(start + 128, width), :].astype(f32)
        r.tok[:, start : min(start + 128, width)] = jnp.transpose(part).astype(bf16)
    ready(-1, gain)
    values = r.tok[...].astype(f32)
    mean_sq = jnp.mean(values * values, axis=-1, keepdims=True)
    r.normed[...] = (
        values * lax.rsqrt(mean_sq + norm_eps) * gain[...][None, :]
    ).astype(bf16)
    for index, ref in enumerate(r.small[1:]):
        ready(-2 - index, ref)
    row = lax.broadcasted_iota(jnp.int32, (rows, rows), 0)
    col = lax.broadcasted_iota(jnp.int32, (rows, rows), 1)
    offset = row - col
    across_row = seg_row[...].astype(f32)
    down = jnp.transpose(jnp.broadcast_to(across_row, (128, rows)))
    down = jnp.concatenate([down] * (rows // 128), axis=1)
    allowed = (down == across_row) & (offset >= 0) & (offset < WINDOW)
    r.mask[...] = jnp.where(allowed, 1.0, 0.0)

    def project(start):
        size = min(256, r.w_q.shape[0] - start)
        r.proj[:, start : start + size] = lax.dot_general(
            r.normed[...], r.w_q[start : start + size, :], (((1,), (1,)), ((), ())),
            preferred_element_type=f32,
        )

    lane = lax.broadcasted_iota(jnp.int32, (rows, 128), 1)
    low = lane < HEAD_DIM
    q_rows = cfg.heads * HEAD_DIM
    kv_rows = cfg.kv_heads * HEAD_DIM
    repeat = cfg.heads // cfg.kv_heads
    kept = {}

    def attend(slab):
        allowed = r.mask[...] > 0.0
        zero = jnp.zeros((rows, 128), f32)
        group = slab * 2 // repeat
        if group not in kept:
            base = q_rows + group // 2 * 128
            keys = r.proj[:, base : base + 128]
            keys = keys * cosine[...] + swap_halves(keys, lane) * sine[...]
            vals = r.proj[:, base + kv_rows : base + kv_rows + 128]
            keys_turned, vals_turned = pltpu.roll(keys, HEAD_DIM, 1), pltpu.roll(vals, HEAD_DIM, 1)
            if group % 2 == 1:
                keys, keys_turned, vals, vals_turned = keys_turned, keys, vals_turned, vals
            kept[group] = (
                (jnp.where(low, keys, zero).astype(bf16), jnp.where(low, vals, zero).astype(bf16)),
                (
                    jnp.where(low, zero, keys_turned).astype(bf16),
                    jnp.where(low, zero, vals_turned).astype(bf16),
                ),
            )
        query = r.proj[:, slab * 128 : slab * 128 + 128]
        query = (query * cosine[...] + swap_halves(query, lane) * sine[...]).astype(bf16)
        total = None
        for which, (key_side, val_side) in enumerate(kept[group]):
            scores = lax.dot_general(
                query, key_side, (((1,), (1,)), ((), ())), preferred_element_type=f32
            ) * (HEAD_DIM**-0.5)
            weights = jnp.where(allowed, jnp.exp(scores), 0.0)
            sink = jnp.exp(jnp.full((rows, 1), sinks[2 * slab + which]))
            running = sink + jnp.sum(weights, axis=-1, keepdims=True)
            probs = (weights * (1.0 / running)).astype(bf16)
            part = jnp.dot(probs, val_side, preferred_element_type=f32)
            total = part if total is None else total + part
        r.att[:, slab * 128 : slab * 128 + 128] = total.astype(bf16)

    ours = pl.ds(pl.multiple_of(side * half, half), half)
    theirs = pl.ds(pl.multiple_of(across * half, half), half)

    def swap_copy(index):
        return pltpu.make_async_remote_copy(
            src_ref=r.swap_out[index], dst_ref=r.swap_in[index],
            send_sem=r.swap_send.at[index], recv_sem=r.swap_recv.at[index],
            device_id={"dp": across}, device_id_type=MESH,
        )

    def product(index, which):
        start, size = cfg.segments[index]
        for at in range(0, size, 512):
            span = min(512, size - at)
            part = jnp.dot(
                r.att[ours if which else theirs, :], r.o_part[index][:, at : at + span],
                preferred_element_type=f32,
            )
            if which:
                total = r.tok[ours, start + at : start + at + span].astype(f32) + part
                r.res[:, start + at : start + at + span] = total
            else:
                r.swap_out[index][:, at : at + span] = part.astype(bf16)

    def swap(index):
        product(index, 0)
        swap_copy(index).start()
        product(index, 1)

    def receive(index):
        start, size = cfg.segments[index]
        landed(r.swap_in[index], r.swap_recv.at[index])
        r.res[:, start : start + size] += r.swap_in[index][...].astype(f32)

    heads_slabs = cfg.heads // 2
    spans = range(0, r.w_q.shape[0], 256)

    def unpack_tails():
        part = r.o_part[-1]
        edge = part.shape[1] - 64
        for slot in range(2 * chips):
            low_half, high_half = slice(0, 64), slice(64, 128)
            at = slot * q_block
            r.w_q[at : at + upper, full:] = r.tails[slot, :upper, low_half]
            r.w_q[at + upper : at + q_block, full:] = r.tails[slot, : q_block - upper, high_half]
            at = slot * o_block
            part[at : at + lower, edge:] = r.tails[slot, upper:, low_half]
            part[at + lower : at + o_block, edge:] = r.tails[slot, upper:, high_half]

    advance(0, 1)
    advance(1, 1)
    own_sends(2)
    for step in range(2, hops):
        advance(0, step)
        advance(1, step)
        advance(2, step - 1)
    own_sends(3)
    advance(0, hops)
    advance(1, hops)
    all_here(0)
    all_here(1)
    unpack_tails()
    for start in spans[:3]:
        project(start)
    advance(2, hops - 1)
    own_sends(4)
    for start in spans[3:]:
        project(start)
    for slab in range(heads_slabs // 2):
        attend(slab)
    advance(3, 1)
    for slab in range(heads_slabs // 2, heads_slabs):
        attend(slab)
    advance(2, hops)
    advance(4, 1)
    all_here(2)
    swap(0)
    advance(3, 2)
    advance(4, 2)
    advance(3, 3)
    receive(0)
    r.rows_a[me] = r.res[:, :cut].astype(bf16)
    early, late = (0, half // 4), (half // 2, 3 * half // 4)
    own_sends(fast, early, False)
    advance(4, 3)
    own_sends(fast, late)
    advance(3, 4)
    all_here(3)
    swap(1)
    advance(fast, 1, early)
    advance(4, 4)
    all_here(4)
    swap(2)
    advance(fast, 1, late)
    receive(1)
    advance(fast, 2)
    receive(2)

    experts = router.shape[0]
    top_count = cfg.top_count
    residual = r.res[...]
    mean_sq = jnp.mean(residual * residual, axis=-1, keepdims=True)
    scale = lax.rsqrt(mean_sq + norm_eps)
    head = (r.res[:, :cut] * scale * mlp[:cut][None, :]).astype(bf16)
    tail = (r.res[:, cut:] * scale * mlp[cut:][None, :]).astype(bf16)
    r.rows_b[me] = tail
    edge = tail.shape[1] - 64
    quiet = r.notes.shape[1] - half // 2
    r.notes[me, quiet:, :64] = tail[: half // 2, edge:]
    r.notes[me, quiet:, 64:] = tail[half // 2 :, edge:]
    across_lanes = (((1,), (1,)), ((), ()))
    logits = (
        lax.dot_general(router[:, :cut], head, across_lanes, preferred_element_type=f32)
        + lax.dot_general(router[:, cut:], tail, across_lanes, preferred_element_type=f32)
        + jnp.transpose(jnp.broadcast_to(bias[...], (half, experts)))
    )
    ids = ids_ref[:, ours]
    expert = lax.broadcasted_iota(jnp.int32, (experts, half), 0)
    picked = [ids[k : k + 1, :] == expert for k in range(top_count)]
    hit = sum(jnp.where(p, 1.0, 0.0) for p in picked)
    earlier = lax.broadcasted_iota(jnp.int32, (half, half), 0) < lax.broadcasted_iota(
        jnp.int32, (half, half), 1
    )
    before = jnp.dot(
        hit.astype(bf16), jnp.where(earlier, 1.0, 0.0).astype(bf16), preferred_element_type=f32
    )
    raised = [jnp.exp(jnp.sum(jnp.where(p, logits, 0.0), axis=0, keepdims=True)) for p in picked]
    share = 1.0 / sum(raised)
    line = lax.broadcasted_iota(jnp.int32, (quiet, half), 0)
    note = jnp.zeros(line.shape, f32)
    for k in range(top_count):
        slot = jnp.sum(jnp.where(picked[k], before, 0.0), axis=0, keepdims=True)
        note = jnp.where(line == k, raised[k] * share, note)
        note = jnp.where(line == top_count + k, ids[k : k + 1, :].astype(f32), note)
        note = jnp.where(line == 2 * top_count + k, slot, note)
    rest = jnp.transpose(jnp.broadcast_to(scale, (half, 128)))[:1, :]
    for k in range(3):
        term = rest.astype(bf16).astype(f32)
        note = jnp.where(line == 3 * top_count + k, term, note)
        rest = rest - term
    r.notes[me, :quiet] = note.astype(bf16)

    def take(slot):
        own_expert = me.astype(f32)
        note = r.notes[slot, :quiet].astype(f32)
        r.rows_b[slot, : half // 2, edge:] = r.notes[slot, quiet:, :64]
        r.rows_b[slot, half // 2 :, edge:] = r.notes[slot, quiet:, 64:]
        gate = jnp.zeros((1, half), f32)
        where_to = jnp.full((1, half), -1.0, f32)
        for k in range(top_count):
            chosen = note[top_count + k : top_count + k + 1, :] == own_expert
            gate = jnp.where(chosen, note[k : k + 1, :], gate)
            where_to = jnp.where(chosen, note[2 * top_count + k : 2 * top_count + k + 1, :], where_to)
        at = 3 * top_count
        scales = note[at : at + 1, :] + note[at + 1 : at + 2, :] + note[at + 2 : at + 3, :]
        match = lax.broadcasted_iota(jnp.int32, (capacity, half), 0).astype(f32) == where_to
        select = jnp.where(match, 1.0, 0.0).astype(bf16)
        gates = lax.dot_general(
            jnp.broadcast_to(gate, (8, half)).astype(bf16), select, across_lanes,
            preferred_element_type=f32,
        )
        r.gate_rows[slot] = gates[:1, :]
        scales = jnp.sum(jnp.where(match, scales, 0.0), axis=1, keepdims=True)
        r.out[slot, :, cut:] = jnp.dot(
            select, r.rows_b[slot], preferred_element_type=f32
        ).astype(bf16)
        r.out[slot, :, :cut] = (
            jnp.dot(select, r.rows_a[slot], preferred_element_type=f32)
            * scales * mlp[:cut][None, :]
        ).astype(bf16)

    own_sends(marks)
    own_sends(slow)
    advance(fast, 3)
    take(me)

    def ring_task(way, step):
        return lambda: take(origin(way, step))

    def pair_task(ways, step):
        def run():
            for group in (fast, slow, marks):
                pair_wait(group, ways[0], step)
            take(origin(ways[0], step) + flip)
        return run

    def partner_task():
        for group in (fast, slow, marks):
            pair_wait(group, 1, 0)
        take(partner)

    tasks.append(partner_task)
    for step in range(1, hops + 1):
        advance(marks, step)
        advance(slow, step)
        if step == 1:
            advance(fast, 4)
        for ways in ((1,), (-1,)) if step < hops else ((1, -1),):
            tasks.append(ring_task(ways[0], step))
            tasks.append(pair_task(ways, step))
    while tasks:
        tasks.pop(0)()
    r.gates[...] = r.gate_rows[:, 0, :].astype(bf16)

    for group in range(marks + 1):
        landed(blocks(group, chips - 1), r.ring_send.at[group])
        landed(blocks(group, chips), r.pair_send.at[group])
    for index in range(swaps):
        swap_copy(index).wait_send()


def write_kernel(pieces, out_ref, gate_ref, out_hbm, gate_hbm, sems):
    share = out_ref.shape[0] // pieces
    copies = [pltpu.make_async_copy(gate_ref, gate_hbm, sems.at[pieces])]
    for piece in range(pieces):
        part = pl.ds(piece * share, share)
        copies.append(pltpu.make_async_copy(out_ref.at[part], out_hbm.at[part], sems.at[piece]))
    for copy in copies:
        copy.start()
    for copy in copies:
        copy.wait()


def write_call(out, gates, pieces):
    vmem, hbm = (pl.BlockSpec(memory_space=kind) for kind in (pltpu.VMEM, pltpu.HBM))
    return pl.pallas_call(
        functools.partial(write_kernel, pieces),
        out_shape=[pltpu.HBM(v.shape, v.dtype) for v in (out, gates)],
        in_specs=[vmem] * 2,
        out_specs=[hbm] * 2,
        scratch_shapes=[pltpu.SemaphoreType.DMA((pieces + 1,))],
        compiler_params=pltpu.CompilerParams(vmem_limit_bytes=2 * 1024 * 1024),
        name="write_out",
    )(out, gates)


def layer_call(
    tokens, segments, expert_ids, gain, sinks, adam, router_weight, router_bias, mlp_gain,
    heads, kv_heads, sources, experts, capacity,
):
    rows, width = tokens.shape
    half = rows // 2
    chips = sources // 2
    hops = chips // 2
    q_block, o_block = adam[0].shape[0], adam[4].shape[0]
    top_count = expert_ids.shape[1]
    cut = width * 3 // 8 // 128 * 128
    segments_o = ((0, cut), (cut, cut), (2 * cut, width - 2 * cut))
    tiles = q_block // 16
    top = (tiles + 1) // 2 * 16
    q_spans = [(0, 32, 1), (32, top - 32, 1), (top, q_block - top, -1)]
    o_spans = [(0, o_block // 2, 1), (o_block // 2, o_block // 2, -1)]
    last_spans = [(0, 16, 1), (16, o_block - 16, -1)]
    quarter = half // 4
    r_spans = [(quarter * t, quarter, 1 if t < 2 else -1) for t in range(4)]
    tops = (q_block + 31) // 32 * 16, o_block // 2
    tail_rows, note_rows = sum(tops), 16 + half // 2

    spans = (
        q_spans, [(0, tail_rows, -1)], o_spans, o_spans, last_spans, r_spans, r_spans,
        [(0, note_rows, 1)],
    )
    plan, total = piece_plan(spans, hops)
    cosine, sine = split_tables(rows)
    bf16, f32 = jnp.bfloat16, jnp.float32
    hbm = dict(
        tok=tokens.T, adam=adam,
        small=[
            gain, mlp_gain, segments[None, :], jnp.asarray(cosine), jnp.asarray(sine),
            router_weight.T, router_bias[None, :], expert_ids.T, sinks,
        ],
    )
    small = [pltpu.VMEM(v.shape, v.dtype) for v in hbm["small"][:-1]]
    dma = pltpu.SemaphoreType.DMA
    groups, swaps = len(spans), len(segments_o)
    scratch = dict(
        tok=pltpu.VMEM(tokens.shape, bf16),
        tok_t=pltpu.VMEM((width, rows), bf16),
        small=small + [pltpu.SMEM(sinks.shape, sinks.dtype)],
        mask=pltpu.VMEM((rows, rows), f32),
        q_in=pltpu.VMEM((4, q_block, width), f32),
        o_in=pltpu.VMEM((4, o_block, width), f32),
        normed=pltpu.VMEM((rows, width), bf16),
        w_q=pltpu.VMEM((sources * q_block, width), bf16),
        tails=pltpu.VMEM((sources, tail_rows, 128), bf16),
        o_part=[pltpu.VMEM((sources * o_block, size), bf16) for _, size in segments_o],
        proj=pltpu.VMEM((rows, sources * q_block), f32),
        att=pltpu.VMEM((rows, heads * HEAD_DIM), bf16),
        res=pltpu.VMEM((half, width), f32),
        swap_out=[pltpu.VMEM((half, size), bf16) for _, size in segments_o],
        swap_in=[pltpu.VMEM((half, size), bf16) for _, size in segments_o],
        rows_a=pltpu.VMEM((sources, half, cut), bf16),
        rows_b=pltpu.VMEM((sources, half, width - cut), bf16),
        notes=pltpu.VMEM((sources, note_rows, half), bf16),
        gate_rows=pltpu.VMEM((sources, 1, capacity), f32),
        load_sem=dma((tiles + 11,)),
        ring_send=dma((groups,)),
        ring_recv=dma((total,)),
        pair_send=dma((groups,)),
        pair_recv=dma((groups - 3 + 3 * chips,)),
        swap_send=dma((swaps,)),
        swap_recv=dma((swaps,)),
    )
    results = dict(
        out=pltpu.VMEM((sources, capacity, width), bf16),
        gates=pltpu.VMEM((sources, capacity), bf16),
    )
    operands, hbm_tree = jax.tree.flatten(hbm)
    outputs, result_tree = jax.tree.flatten(results)
    buffers, scratch_tree = jax.tree.flatten(scratch)
    own = (q_block, tail_rows, *[o_block] * swaps, half, half, note_rows)
    cfg = types.SimpleNamespace(
        plan=plan, own=own, chips=chips, heads=heads, kv_heads=kv_heads, segments=segments_o,
        top_count=top_count, tops=tops,
    )

    def body(*refs):
        taken = list(refs)
        spaces = []
        for tree in (hbm_tree, result_tree, scratch_tree):
            count = tree.num_leaves
            spaces.append(jax.tree.unflatten(tree, taken[:count]))
            taken = taken[count:]
        layer_kernel(
            cfg, types.SimpleNamespace(**spaces[0]),
            types.SimpleNamespace(**spaces[1], **spaces[2]),
        )

    gates, out = pl.pallas_call(
        body,
        out_shape=outputs,
        in_specs=[pl.BlockSpec(memory_space=pltpu.HBM)] * len(operands),
        out_specs=[pl.BlockSpec(memory_space=pltpu.VMEM)] * 2,
        scratch_shapes=buffers,
        compiler_params=pltpu.CompilerParams(
            collective_id=4, has_side_effects=True, vmem_limit_bytes=48 * 1024 * 1024
        ),
        name="layer",
    )(*(pltpu.with_memory_space_constraint(v, pltpu.HBM) for v in operands))
    return write_call(out, gates, 8)


def layer_fits(tokens, adam, sources, experts, capacity, groups):
    rows, width = tokens.shape
    return (
        groups == 2 and experts == sources and sources == 16 and rows == 256
        and adam[0].shape[0] % 16 == 0 and adam[0].shape[0] >= 80 and adam[4].shape[0] % 32 == 0
        and width % 128 == 64 and width >= 1024 and capacity <= 128
    )


def on_device(
    tokens,
    segment_ids,
    expert_ids,
    attn_gain,
    sinks,
    qkv_master,
    qkv_mom,
    qkv_var,
    qkv_grad,
    o_master,
    o_mom,
    o_var,
    o_grad,
    router_weight,
    router_bias,
    mlp_gain,
):
    tok_rows, width = tokens.shape
    half = tok_rows // lax.axis_size("dp")
    sources = lax.axis_size("expert")
    heads_here = sinks.shape[0]
    kv_here = KV_HEADS * heads_here // HEADS
    experts = router_weight.shape[1]
    top_count = expert_ids.shape[1]
    capacity = 2 * half * top_count // experts
    adam = [qkv_master, qkv_mom, qkv_var, qkv_grad, o_master, o_mom, o_var, o_grad]
    if layer_fits(tokens, adam, sources, experts, capacity, lax.axis_size("dp")):
        dispatched, gate_slots = layer_call(
            tokens, segment_ids, expert_ids, attn_gain, sinks, adam, router_weight, router_bias,
            mlp_gain, heads_here, kv_here, sources, experts, capacity,
        )
        return (dispatched[None, :, None], gate_slots[None, :, None])
    qkv_local = adam_weights(qkv_master, qkv_mom, qkv_var, qkv_grad)
    o_local = adam_weights(o_master, o_mom, o_var, o_grad)
    qkv_full, o_full = gather_rows([qkv_local, o_local], sources, 1)
    part = attention_call(
        tokens, attn_gain, qkv_full, o_full, segment_ids, sinks, heads_here, kv_here
    ).reshape(-1, half, width)
    got = exchange_call(part, 2)
    rows = router_call(
        tokens, part, got, mlp_gain, router_weight, router_bias, expert_ids, 128 - width % 128
    )
    compact = sources * half <= 2 * experts * capacity
    if experts == sources and compact and ring_fits([rows], sources):
        dispatched, gate_slots = ring_gather(
            [rows], 4, sources, 3, (top_count, capacity, width)
        )
        return (dispatched[None, :, None], gate_slots[None])
    return exchange_slots(rows, width, experts, capacity, top_count, sources)


def solution(mesh):
    return jax.shard_map(
        on_device,
        mesh=mesh,
        in_specs=(
            P("expert", None),
            P("expert"),
            P("expert", None),
            P(),
            P("dp"),
            P(("dp", "expert"), None),
            P(("dp", "expert"), None),
            P(("dp", "expert"), None),
            P(("dp", "expert"), None),
            P(("dp", "expert"), None),
            P(("dp", "expert"), None),
            P(("dp", "expert"), None),
            P(("dp", "expert"), None),
            P(),
            P(),
            P(),
        ),
        out_specs=(P("expert", None, "dp", None, None), P("expert", None, "dp", None)),
        check_vma=False,
    )
```

```python
import functools
import types

import jax
import jax.numpy as jnp
import numpy as np
from jax import lax
from jax.experimental import pallas as pl
from jax.experimental.pallas import tpu as pltpu
from jax.sharding import PartitionSpec as P

HEADS = 32
KV_HEADS = 4
HEAD_DIM = 64
WINDOW = 128
MESH = pl.DeviceIdType.MESH
VMEM_BYTES = 36 * 1024 * 1024


beta_one = 0.9
beta_two = 0.999
adam_step = 100
learn_rate = 0.02
adam_eps = 1e-08
norm_eps = 1e-05
rope_base = 150000.0


def adam_weights(master, moment, second_mom, gradient):
    moment_new = beta_one * moment + (1.0 - beta_one) * gradient
    second_new = beta_two * second_mom + (1.0 - beta_two) * gradient * gradient
    fix_one = 1.0 - beta_one**adam_step
    fix_two = 1.0 - beta_two**adam_step
    update = moment_new / fix_one / (jnp.sqrt(second_new / fix_two) + adam_eps)
    return (master - learn_rate * update).astype(jnp.bfloat16)


def rotation_tables(rows):
    half_dim = HEAD_DIM // 2
    positions = jnp.arange(rows).astype(jnp.float32)
    frequency = rope_base ** (-(jnp.arange(half_dim).astype(jnp.float32) * 2.0) / HEAD_DIM)
    angles = positions[:, None] * frequency[None, :]
    cosine = jnp.cos(angles)
    sine = jnp.sin(angles)
    return (
        jnp.concatenate([cosine] * 4, axis=1),
        jnp.concatenate([-sine, sine, -sine, sine], axis=1),
    )


def chip_at(place, chips):
    place = lax.rem(place + 2 * chips, chips)
    return jnp.where(place < chips // 2, 2 * place, 2 * (chips - 1 - place) + 1)


def gather_kernel(chips, plan, top_count, *refs):
    count = len({entry[0] for entry in plan})
    if top_count:
        (source, out_ref, gate_ref, held), sems = refs[:4], refs[4:]
        ins, outs = (source,), (held,)
    else:
        ins, outs, sems = refs[:count], refs[count : 2 * count], refs[2 * count :]
    ring_send, ring_recv, pair_send, pair_recv, own_send, own_recv, own_sem = sems
    me = lax.axis_index("expert")
    core = lax.rem(me, 2)
    chip = me // 2
    place = jnp.where(lax.rem(chip, 2) == 0, chip // 2, chips - 1 - chip // 2)
    right = chip_at(place + 1, chips) * 2 + core
    left = chip_at(place - 1, chips) * 2 + core
    partner = me + 1 - 2 * core

    barrier = pltpu.get_barrier_semaphore()
    for other in (left, right, partner):
        pl.semaphore_signal(barrier, inc=1, device_id={"expert": other}, device_id_type=MESH)
    pl.semaphore_wait(barrier, 3)

    def block(j, slot):
        arr, start, size = plan[j][:3]
        return outs[arr].at[slot, pl.ds(start, size)]

    def origin(way, step):
        return chip_at(place - step if way > 0 else place + step, chips) * 2 + core

    def copy_to(j, step, send, recv, target):
        arr, start, size, way, _ = plan[j]
        slot = origin(way, step)
        return pltpu.make_async_remote_copy(
            src_ref=ins[arr].at[pl.ds(start, size)] if step == 0 else block(j, slot),
            dst_ref=block(j, slot),
            send_sem=send.at[j, step],
            recv_sem=recv.at[j, step],
            device_id={"expert": target},
            device_id_type=MESH,
        )

    def ring_copy(j, step):
        return copy_to(j, step, ring_send, ring_recv, right if plan[j][3] > 0 else left)

    def pair_copy(j, step):
        return copy_to(j, step, pair_send, pair_recv, partner)

    def own_copy(arr, slot):
        return pltpu.make_async_remote_copy(
            src_ref=ins[arr],
            dst_ref=outs[arr].at[slot],
            send_sem=own_send.at[arr],
            recv_sem=own_recv.at[arr],
            device_id={"expert": partner},
            device_id_type=MESH,
        )

    def landed(j, slot, sem):
        pltpu.make_async_copy(block(j, slot), block(j, slot), sem).wait()

    def consume(rows, slot):
        if top_count:
            fill_slots(top_count, rows, out_ref, gate_ref, slot)

    def take_mine():
        consume(ins[0], me)

    def take_partner():
        for arr in range(count):
            pltpu.make_async_copy(
                outs[arr].at[partner], outs[arr].at[partner], own_recv.at[arr]
            ).wait()
        consume(outs[0].at[partner], partner)

    def take_ring(way, step):
        slot = origin(way, step)
        consume(outs[0].at[slot], slot)

    def take_pair(ways, step):
        for j, entry in enumerate(plan):
            if entry[3] in ways and step <= entry[4]:
                landed(j, origin(entry[3], step) + 1 - 2 * core, pair_recv.at[j, step])
        slot = origin(ways[0], step) + 1 - 2 * core
        consume(outs[0].at[slot], slot)

    every = range(len(plan))
    hops = chips // 2
    for j in every:
        ring_copy(j, 0).start()
    for arr in range(count):
        own_copy(arr, me).start()
    owns = []
    if not top_count:
        owns = [
            pltpu.make_async_copy(ins[a], outs[a].at[me], own_sem.at[a]) for a in range(count)
        ]
    for copy in owns:
        copy.start()
    tasks = [take_mine, take_partner]
    for step in range(1, hops + 1):
        for j in every:
            if step > plan[j][4]:
                continue
            landed(j, origin(plan[j][3], step), ring_recv.at[j, step - 1])
            if step < plan[j][4]:
                ring_copy(j, step).start()
            pair_copy(j, step).start()
            if tasks:
                tasks.pop(0)()
        for ways in ((1,), (-1,)) if step < hops else ((1, -1),):
            tasks.append(functools.partial(take_ring, ways[0], step))
            tasks.append(functools.partial(take_pair, ways, step))
    tasks = tasks[::2] + tasks[1::2]
    for task in tasks:
        task()
    for copy in owns:
        copy.wait()
    for arr in range(count):
        own_copy(arr, me).wait_send()
    for j in every:
        for step in range(plan[j][4] + 1):
            if step:
                pair_copy(j, step).wait_send()
            if step < plan[j][4]:
                ring_copy(j, step).wait_send()


def ring_gather(arrays, cuts, sources, call_id, slots=None):
    plan = []
    chips = sources // 2
    for arr, value in enumerate(arrays):
        tiles = value.shape[0] // 16
        for cut in range(cuts):
            start = (tiles * cut + cuts - 1) // cuts * 16
            size = (tiles * (cut + 1) + cuts - 1) // cuts * 16 - start
            for way in (1, -1):
                far = (cut < cuts // 2) == (way > 0)
                plan.append((arr, start, size, way, chips // 2 - (0 if far else 1)))
    copies, count = len(plan), len(arrays)
    gathered = [jax.ShapeDtypeStruct((sources, *v.shape), v.dtype) for v in arrays]
    sems = [pltpu.SemaphoreType.DMA((copies, chips // 2 + 1))] * 4
    sems += [pltpu.SemaphoreType.DMA((count,))] * 3
    vmem = pl.BlockSpec(memory_space=pltpu.VMEM)
    if slots:
        top_count, capacity, width = slots
        out_shape = (
            jax.ShapeDtypeStruct((sources, capacity, width), jnp.bfloat16),
            jax.ShapeDtypeStruct((sources, 1, capacity), jnp.bfloat16),
        )
        out_specs = (vmem, vmem)
        held = [pltpu.VMEM(gathered[0].shape, gathered[0].dtype)]
    else:
        top_count, out_shape, held = 0, gathered, []
        out_specs = [vmem] * count
    return pl.pallas_call(
        functools.partial(gather_kernel, chips, tuple(plan), top_count),
        out_shape=out_shape,
        in_specs=[vmem] * count,
        out_specs=out_specs,
        scratch_shapes=held + sems,
        compiler_params=pltpu.CompilerParams(
            collective_id=call_id, has_side_effects=True,
            vmem_limit_bytes=(40 if slots else 24) * 1024 * 1024,
        ),
        name="ring_slots" if slots else "ring_gather",
    )(*arrays)


def ring_fits(arrays, sources):
    return sources % 4 == 0 and 8 <= sources <= 32 and all(a.shape[0] % 16 == 0 for a in arrays)


def gather_rows(arrays, sources, call_id):
    if ring_fits(arrays, sources):
        width = arrays[0].shape[1]
        return [v.reshape(-1, width) for v in ring_gather(arrays, 2, sources, call_id)]
    return [lax.all_gather(a, "expert", axis=0, tiled=True) for a in arrays]


def swap_halves(values, lane):
    up = pltpu.roll(values, 128 - HEAD_DIM // 2, 1)
    down = pltpu.roll(values, HEAD_DIM // 2, 1)
    return jnp.where(lane % HEAD_DIM < HEAD_DIM // 2, up, down)


def attention_kernel(
    heads, kv_heads, tok_ref, gain_ref, w_ref, o_ref, cos_ref, sin_ref, seg_col, seg_row, sink_ref,
    out_ref, proj_ref, att_ref,
):
    rows = tok_ref.shape[0]
    bf16 = jnp.bfloat16
    values = tok_ref[...].astype(jnp.float32)
    mean_sq = jnp.mean(values * values, axis=-1, keepdims=True)
    normed = (values * lax.rsqrt(mean_sq + norm_eps) * gain_ref[...][None, :]).astype(bf16)
    features = w_ref.shape[0]
    for start in range(0, features, 256):
        size = min(256, features - start)
        proj_ref[:, start : start + size] = lax.dot_general(
            normed, w_ref[start : start + size, :], (((1,), (1,)), ((), ())),
            preferred_element_type=jnp.float32,
        )
    lane = lax.broadcasted_iota(jnp.int32, (rows, 128), 1)
    low = lane < HEAD_DIM
    cosine, sine = cos_ref[...], sin_ref[...]
    row = lax.broadcasted_iota(jnp.int32, (rows, rows), 0)
    col = lax.broadcasted_iota(jnp.int32, (rows, rows), 1)
    offset = row - col
    allowed = (seg_col[...] == seg_row[...]) & (offset >= 0) & (offset < WINDOW)
    q_rows = heads * HEAD_DIM
    kv_rows = kv_heads * HEAD_DIM
    repeat = heads // kv_heads
    zero = jnp.zeros((rows, 128), jnp.float32)
    for group in range(kv_heads):
        base = q_rows + group // 2 * 128
        keys = proj_ref[:, base : base + 128]
        keys = keys * cosine + swap_halves(keys, lane) * sine
        vals = proj_ref[:, base + kv_rows : base + kv_rows + 128]
        keys_turned, vals_turned = pltpu.roll(keys, HEAD_DIM, 1), pltpu.roll(vals, HEAD_DIM, 1)
        if group % 2 == 1:
            keys, keys_turned, vals, vals_turned = keys_turned, keys, vals_turned, vals
        sides = (
            (jnp.where(low, keys, zero).astype(bf16), jnp.where(low, vals, zero).astype(bf16)),
            (
                jnp.where(low, zero, keys_turned).astype(bf16),
                jnp.where(low, zero, vals_turned).astype(bf16),
            ),
        )
        for slab in range(group * repeat // 2, (group + 1) * repeat // 2):
            query = proj_ref[:, slab * 128 : slab * 128 + 128]
            query = (query * cosine + swap_halves(query, lane) * sine).astype(bf16)
            total = None
            for side, (key_side, val_side) in enumerate(sides):
                scores = lax.dot_general(
                    query, key_side, (((1,), (1,)), ((), ())), preferred_element_type=jnp.float32
                ) * (HEAD_DIM**-0.5)
                weights = jnp.where(allowed, jnp.exp(scores), 0.0)
                running = jnp.exp(jnp.full((rows, 1), sink_ref[2 * slab + side])) + jnp.sum(weights, axis=-1, keepdims=True)
                probs = (weights * (1.0 / running)).astype(bf16)
                part = jnp.dot(probs, val_side, preferred_element_type=jnp.float32)
                total = part if total is None else total + part
            att_ref[:, slab * 128 : slab * 128 + 128] = total.astype(bf16)
    width = o_ref.shape[1]
    for start in range(0, width, 384):
        size = min(384, width - start)
        out_ref[:, start : start + size] = jnp.dot(
            att_ref[...], o_ref[:, start : start + size], preferred_element_type=jnp.float32
        ).astype(bf16)


def attention_call(tokens, gain, qkv_full, o_full, segments, sinks, heads, kv_heads):
    rows, width = tokens.shape
    cosine, sine = rotation_tables(rows)
    vmem = pl.BlockSpec(memory_space=pltpu.VMEM)
    return pl.pallas_call(
        functools.partial(attention_kernel, heads, kv_heads),
        out_shape=jax.ShapeDtypeStruct((rows, width), jnp.bfloat16),
        in_specs=[vmem] * 8 + [pl.BlockSpec(memory_space=pltpu.SMEM)],
        out_specs=vmem,
        scratch_shapes=[
            pltpu.VMEM((rows, qkv_full.shape[0]), jnp.float32),
            pltpu.VMEM((rows, heads * HEAD_DIM), jnp.bfloat16),
        ],
        compiler_params=pltpu.CompilerParams(vmem_limit_bytes=VMEM_BYTES),
        name="attention_part",
    )(
        tokens, gain, qkv_full, o_full, cosine, sine, segments[:, None],
        segments[None, :], sinks,
    )


def exchange_kernel(part_ref, got_ref, send_sem, recv_sem):
    group = lax.axis_index("dp")
    other = 1 - group
    barrier = pltpu.get_barrier_semaphore()
    pl.semaphore_signal(barrier, inc=1, device_id={"dp": other}, device_id_type=MESH)
    pl.semaphore_wait(barrier, 1)
    copy = pltpu.make_async_remote_copy(
        src_ref=part_ref.at[other],
        dst_ref=got_ref,
        send_sem=send_sem,
        recv_sem=recv_sem,
        device_id={"dp": other},
        device_id_type=MESH,
    )
    copy.start()
    copy.wait()


def exchange_call(part, call_id):
    return pl.pallas_call(
        exchange_kernel,
        out_shape=jax.ShapeDtypeStruct(part.shape[1:], part.dtype),
        in_specs=[pl.BlockSpec(memory_space=pltpu.VMEM)],
        out_specs=pl.BlockSpec(memory_space=pltpu.VMEM),
        scratch_shapes=[pltpu.SemaphoreType.DMA, pltpu.SemaphoreType.DMA],
        compiler_params=pltpu.CompilerParams(
            collective_id=call_id, has_side_effects=True, vmem_limit_bytes=16 * 1024 * 1024
        ),
        name="exchange_halves",
    )(part)


def router_kernel(tok_ref, part_ref, got_ref, gain_ref, rw_ref, bias_ref, ids_ref, out_ref):
    group = lax.axis_index("dp")
    half, width = got_ref.shape
    experts = rw_ref.shape[0]
    top_count = ids_ref.shape[1]
    rows = pl.ds(pl.multiple_of(group * half, half), half)
    summed = part_ref[group].astype(jnp.float32) + got_ref[...].astype(jnp.float32)
    residual = tok_ref[rows, :].astype(jnp.float32) + summed
    mean_sq = jnp.mean(residual * residual, axis=-1, keepdims=True)
    moe_in = (residual * lax.rsqrt(mean_sq + norm_eps) * gain_ref[...][None, :]).astype(jnp.bfloat16)
    out_ref[:, :width] = moe_in
    logits = lax.dot_general(
        moe_in, rw_ref[...], (((1,), (1,)), ((), ())), preferred_element_type=jnp.float32
    ) + bias_ref[...]
    ids = ids_ref[rows, :]
    expert = lax.broadcasted_iota(jnp.int32, (half, experts), 1)
    picked = [ids[:, k : k + 1] == expert for k in range(top_count)]
    hit = sum(jnp.where(p, 1.0, 0.0) for p in picked)
    above = lax.broadcasted_iota(jnp.int32, (half, half), 0) > lax.broadcasted_iota(
        jnp.int32, (half, half), 1
    )
    before = jnp.dot(
        jnp.where(above, 1.0, 0.0).astype(jnp.bfloat16), hit.astype(jnp.bfloat16),
        preferred_element_type=jnp.float32,
    )
    raised = [jnp.exp(jnp.sum(jnp.where(p, logits, 0.0), axis=1, keepdims=True)) for p in picked]
    scale = 1.0 / sum(raised)
    column = lax.broadcasted_iota(jnp.int32, (half, out_ref.shape[1] - width), 1)
    extra = jnp.zeros(column.shape, jnp.float32)
    for k in range(top_count):
        slot = jnp.sum(jnp.where(picked[k], before, 0.0), axis=1, keepdims=True)
        extra = jnp.where(column == 3 * k, raised[k] * scale, extra)
        extra = jnp.where(column == 3 * k + 1, ids[:, k : k + 1].astype(jnp.float32), extra)
        extra = jnp.where(column == 3 * k + 2, slot, extra)
    out_ref[:, width:] = extra.astype(jnp.bfloat16)


def router_call(tokens, part, got, gain, router_weight, router_bias, expert_ids, extra):
    half, width = got.shape
    return pl.pallas_call(
        router_kernel,
        out_shape=jax.ShapeDtypeStruct((half, width + extra), jnp.bfloat16),
        in_specs=[pl.BlockSpec(memory_space=pltpu.VMEM)] * 7,
        out_specs=pl.BlockSpec(memory_space=pltpu.VMEM),
        compiler_params=pltpu.CompilerParams(vmem_limit_bytes=VMEM_BYTES),
        name="router_part",
    )(tokens, part, got, gain, router_weight.T, router_bias[None, :], expert_ids)


def fill_slots(top_count, rows_ref, out_ref, gate_ref, slot):
    mine = lax.axis_index("expert").astype(jnp.float32)
    _, capacity, width = out_ref.shape
    half, full = rows_ref.shape
    extra = rows_ref[:, full - 128 :].astype(jnp.float32)
    shift = 128 - (full - width)
    place = lax.broadcasted_iota(jnp.int32, (half, capacity), 1).astype(jnp.float32)
    select = jnp.zeros((half, capacity), jnp.float32)
    gates = jnp.zeros((half, capacity), jnp.float32)
    for k in range(top_count):
        at = shift + 3 * k
        match = (extra[:, at + 1 : at + 2] == mine) & (extra[:, at + 2 : at + 3] == place)
        select = jnp.where(match, 1.0, select)
        gates = jnp.where(match, extra[:, at : at + 1], gates)
    gate_ref[slot] = jnp.sum(gates, axis=0, keepdims=True).astype(jnp.bfloat16)
    out_ref[slot] = lax.dot_general(
        select.astype(jnp.bfloat16), rows_ref[:, :width], (((0,), (0,)), ((), ())),
        preferred_element_type=jnp.float32,
    ).astype(jnp.bfloat16)


def exchange_slots(rows, width, experts, capacity, top_count, sources):
    half = rows.shape[0]
    extra = rows[:, width:].astype(jnp.float32)
    moe_in = rows[:, :width]
    gates, ids, slots = (extra[:, i : 3 * top_count : 3] for i in range(3))
    target = (ids * capacity + slots).astype(jnp.int32).reshape(-1)
    matches = target[None, :] == jnp.arange(experts * capacity, dtype=jnp.int32)[:, None]
    token_match = jnp.any(matches.reshape(experts * capacity, half, top_count), axis=2)
    payload = jnp.dot(
        token_match.astype(jnp.bfloat16), moe_in, preferred_element_type=jnp.float32
    ).astype(jnp.bfloat16)
    slot_gates = jnp.sum(jnp.where(matches, gates.reshape(-1)[None, :], 0.0), axis=1)
    outgoing = (
        payload.reshape(experts, capacity, width),
        slot_gates.astype(jnp.bfloat16).reshape(experts, capacity),
    )
    got_rows, got_gates = (
        lax.all_to_all(v, "expert", split_axis=0, concat_axis=0, tiled=True) for v in outgoing
    )
    per_device = experts // sources
    got_rows = got_rows.reshape(sources, per_device, capacity, width)
    got_gates = got_gates.reshape(sources, per_device, capacity)
    return (
        jnp.transpose(got_rows, (1, 0, 2, 3))[:, :, None],
        jnp.transpose(got_gates, (1, 0, 2))[:, :, None],
    )


def split_tables(rows):
    half_dim = HEAD_DIM // 2
    positions = np.arange(rows).astype(np.float64)
    powers = -(np.arange(half_dim).astype(np.float64) * 2.0) / HEAD_DIM
    frequency = (rope_base**powers).astype(np.float32).astype(np.float64)
    angles = (positions[:, None] * frequency[None, :]).astype(np.float32).astype(np.float64)
    cosine, sine = np.cos(angles), np.sin(angles)
    return (
        np.concatenate([cosine] * 4, axis=1).astype(np.float32),
        np.concatenate([-sine, sine, -sine, sine], axis=1).astype(np.float32),
    )


def piece_plan(groups, hops):
    plan, base = [], 0
    for group, spans in enumerate(groups):
        for start, size, far_way in spans:
            for way in (1, -1):
                count = hops if way == far_way else hops - 1
                plan.append((group, start, size, way, count, base))
                base += count
    return tuple(plan), base


def layer_kernel(cfg, hbm, r):
    bf16, f32 = jnp.bfloat16, jnp.float32
    chips, plan = cfg.chips, cfg.plan
    hops = chips // 2
    me = lax.axis_index("expert")
    side = lax.axis_index("dp")
    core = lax.rem(me, 2)
    chip = me // 2
    place = jnp.where(lax.rem(chip, 2) == 0, chip // 2, chips - 1 - chip // 2)
    right = chip_at(place + 1, chips) * 2 + core
    left = chip_at(place - 1, chips) * 2 + core
    flip = 1 - 2 * core
    partner = me + flip
    across = 1 - side
    rows, width = r.tok.shape
    half = rows // 2
    q_block = r.q_in.shape[1]
    o_block = r.o_in.shape[1]
    capacity = r.out.shape[1]
    cut = cfg.segments[0][1]

    names = []

    def load(name, pairs):
        for src, dst in pairs:
            pltpu.make_async_copy(src, dst, r.load_sem.at[len(names)]).start()
        names.append(name)

    def ready(name, ref):
        pltpu.make_async_copy(ref, ref, r.load_sem.at[names.index(name)]).wait()

    def tile_of(start):
        return r.q_in.at[:, pl.ds(start, 16)]

    for start in range(0, q_block, 16):
        part = pl.ds(start, 16)
        load(start, [(hbm.adam[i].at[part], r.q_in.at[i, part]) for i in range(4)])
    load("tok", [(hbm.tok, r.tok_t)])
    load("o", [(hbm.adam[4 + i], r.o_in.at[i]) for i in range(4)])
    for index, pair in enumerate(zip(hbm.small, r.small)):
        load(-1 - index, [pair])
    gain, mlp, seg_row, cosine, sine, router, bias, ids_ref, sinks = r.small

    barrier = pltpu.get_barrier_semaphore()
    for other in (left, right, partner):
        pl.semaphore_signal(barrier, inc=1, device_id={"expert": other}, device_id_type=MESH)
    pl.semaphore_signal(barrier, inc=1, device_id={"dp": across}, device_id_type=MESH)

    swaps = len(cfg.segments)
    fast, slow, marks = swaps + 2, swaps + 3, swaps + 4
    full = width // 128 * 128
    held = (r.w_q, r.tails, *r.o_part, r.rows_a, r.rows_b, r.notes)
    stride = (q_block, 0, *[o_block] * swaps, 0, 0, 0)

    def block(group, slot, start, size):
        ref = held[group]
        columns = pl.ds(0, ref.shape[-1] // 128 * 128)
        if stride[group]:
            first = pl.multiple_of(slot * stride[group] + start, 16)
            return ref.at[pl.ds(first, size), columns]
        return ref.at[slot, pl.ds(start, size), columns]

    def blocks(group, count):
        if stride[group]:
            return block(group, 0, 0, count * stride[group])
        columns = pl.ds(0, held[group].shape[-1] // 128 * 128)
        return held[group].at[pl.ds(0, count), :, columns]

    def origin(way, step):
        return chip_at(place - step if way > 0 else place + step, chips) * 2 + core

    def send(ref, device, out_sem, in_sem):
        return pltpu.make_async_remote_copy(
            src_ref=ref, dst_ref=ref, send_sem=out_sem, recv_sem=in_sem,
            device_id={"expert": device}, device_id_type=MESH,
        )

    def ring_copy(entry, step):
        group, start, size, way, _, base = entry
        return send(
            block(group, origin(way, step), start, size), right if way > 0 else left,
            r.ring_send.at[group], r.ring_recv.at[base + step],
        )

    def mark(group, way, step):
        if group < fast:
            return group
        at = fast + 2 * hops * (group - fast)
        return at if step == 0 else at + (2 * step - (way > 0) if step < hops else 2 * step - 1)

    def pair_copy(entry, step):
        group, start, size, way, _, _ = entry
        return send(
            block(group, origin(way, step), start, size), partner,
            r.pair_send.at[group], r.pair_recv.at[mark(group, way, step)],
        )

    def own_copy(group):
        return send(
            block(group, me, 0, cfg.own[group]), partner, r.pair_send.at[group],
            r.pair_recv.at[mark(group, 1, 0)],
        )

    def landed(ref, sem):
        pltpu.make_async_copy(ref, ref, sem).wait()

    def entries(group, step):
        return [e for e in plan if e[0] == group and e[4] >= step]

    tasks = []

    def own_sends(group, starts=None, last=True):
        for entry in entries(group, 0):
            if starts is None or entry[1] in starts:
                ring_copy(entry, 0).start()
        if last:
            own_copy(group).start()

    def advance(group, step, starts=None):
        for entry in entries(group, step):
            _, start, size, way, far, base = entry
            if starts is not None and start not in starts:
                continue
            landed(block(group, origin(way, step), start, size), r.ring_recv.at[base + step - 1])
            if step < far:
                ring_copy(entry, step).start()
            pair_copy(entry, step).start()
            if tasks:
                tasks.pop(0)()

    def pair_wait(group, way, step):
        slot = origin(way, step) + flip if step else partner
        landed(block(group, slot, 0, cfg.own[group]), r.pair_recv.at[mark(group, way, step)])

    def all_here(group):
        landed(blocks(group, chips), r.pair_recv.at[group])

    def adam_part(ref, part, columns):
        return adam_weights(*(ref[i, part, columns] for i in range(4)))

    upper = cfg.tops[0]

    def adam_qkv(start):
        ready(start, tile_of(start))
        part = pl.ds(pl.multiple_of(me * q_block + start, 16), 16)
        fresh = adam_part(r.q_in, slice(start, start + 16), slice(None))
        r.w_q[part, :] = fresh
        at, lanes = (start, 0) if start < upper else (start - upper, 64)
        r.tails[me, at : at + 16, lanes : lanes + 64] = fresh[:, full:]

    starts_done = {start + size: (start,) for group, start, size, *_ in plan if group == 0}
    for start in range(0, q_block, 16):
        adam_qkv(start)
        if start == 16:
            pl.semaphore_wait(barrier, 4)
        own_sends(0, starts_done.get(start, ()), False)
    ready("o", r.o_in)
    first = pl.multiple_of(me * o_block, 16)
    for part, (start, size) in zip(r.o_part, cfg.segments):
        fresh = adam_part(r.o_in, slice(None), slice(start, start + size))
        part[pl.ds(first, o_block), :] = fresh
    lower = o_block // 2
    r.tails[me, upper:, :64] = fresh[:lower, size - 64 :]
    r.tails[me, upper:, 64:] = fresh[lower:, size - 64 :]
    own_sends(0, starts_done[q_block])
    own_sends(1)
    ready("tok", r.tok_t)
    for start in range(0, width, 128):
        part = r.tok_t[start : min(start + 128, width), :].astype(f32)
        r.tok[:, start : min(start + 128, width)] = jnp.transpose(part).astype(bf16)
    ready(-1, gain)
    values = r.tok[...].astype(f32)
    mean_sq = jnp.mean(values * values, axis=-1, keepdims=True)
    r.normed[...] = (
        values * lax.rsqrt(mean_sq + norm_eps) * gain[...][None, :]
    ).astype(bf16)
    for index, ref in enumerate(r.small[1:]):
        ready(-2 - index, ref)
    row = lax.broadcasted_iota(jnp.int32, (rows, rows), 0)
    col = lax.broadcasted_iota(jnp.int32, (rows, rows), 1)
    offset = row - col
    across_row = seg_row[...].astype(f32)
    down = jnp.transpose(jnp.broadcast_to(across_row, (128, rows)))
    down = jnp.concatenate([down] * (rows // 128), axis=1)
    allowed = (down == across_row) & (offset >= 0) & (offset < WINDOW)
    r.mask[...] = jnp.where(allowed, 1.0, 0.0)

    def project(start):
        size = min(256, r.w_q.shape[0] - start)
        r.proj[:, start : start + size] = lax.dot_general(
            r.normed[...], r.w_q[start : start + size, :], (((1,), (1,)), ((), ())),
            preferred_element_type=f32,
        )

    lane = lax.broadcasted_iota(jnp.int32, (rows, 128), 1)
    low = lane < HEAD_DIM
    q_rows = cfg.heads * HEAD_DIM
    kv_rows = cfg.kv_heads * HEAD_DIM
    repeat = cfg.heads // cfg.kv_heads
    kept = {}

    def attend(slab):
        allowed = r.mask[...] > 0.0
        zero = jnp.zeros((rows, 128), f32)
        group = slab * 2 // repeat
        if group not in kept:
            base = q_rows + group // 2 * 128
            keys = r.proj[:, base : base + 128]
            keys = keys * cosine[...] + swap_halves(keys, lane) * sine[...]
            vals = r.proj[:, base + kv_rows : base + kv_rows + 128]
            keys_turned, vals_turned = pltpu.roll(keys, HEAD_DIM, 1), pltpu.roll(vals, HEAD_DIM, 1)
            if group % 2 == 1:
                keys, keys_turned, vals, vals_turned = keys_turned, keys, vals_turned, vals
            kept[group] = (
                (jnp.where(low, keys, zero).astype(bf16), jnp.where(low, vals, zero).astype(bf16)),
                (
                    jnp.where(low, zero, keys_turned).astype(bf16),
                    jnp.where(low, zero, vals_turned).astype(bf16),
                ),
            )
        query = r.proj[:, slab * 128 : slab * 128 + 128]
        query = (query * cosine[...] + swap_halves(query, lane) * sine[...]).astype(bf16)
        total = None
        for which, (key_side, val_side) in enumerate(kept[group]):
            scores = lax.dot_general(
                query, key_side, (((1,), (1,)), ((), ())), preferred_element_type=f32
            ) * (HEAD_DIM**-0.5)
            weights = jnp.where(allowed, jnp.exp(scores), 0.0)
            sink = jnp.exp(jnp.full((rows, 1), sinks[2 * slab + which]))
            running = sink + jnp.sum(weights, axis=-1, keepdims=True)
            probs = (weights * (1.0 / running)).astype(bf16)
            part = jnp.dot(probs, val_side, preferred_element_type=f32)
            total = part if total is None else total + part
        r.att[:, slab * 128 : slab * 128 + 128] = total.astype(bf16)

    ours = pl.ds(pl.multiple_of(side * half, half), half)
    theirs = pl.ds(pl.multiple_of(across * half, half), half)

    def swap_copy(index):
        return pltpu.make_async_remote_copy(
            src_ref=r.swap_out[index], dst_ref=r.swap_in[index],
            send_sem=r.swap_send.at[index], recv_sem=r.swap_recv.at[index],
            device_id={"dp": across}, device_id_type=MESH,
        )

    def product(index, which):
        start, size = cfg.segments[index]
        for at in range(0, size, 512):
            span = min(512, size - at)
            part = jnp.dot(
                r.att[ours if which else theirs, :], r.o_part[index][:, at : at + span],
                preferred_element_type=f32,
            )
            if which:
                total = r.tok[ours, start + at : start + at + span].astype(f32) + part
                r.res[:, start + at : start + at + span] = total
            else:
                r.swap_out[index][:, at : at + span] = part.astype(bf16)

    def swap(index):
        product(index, 0)
        swap_copy(index).start()
        product(index, 1)

    def receive(index):
        start, size = cfg.segments[index]
        landed(r.swap_in[index], r.swap_recv.at[index])
        r.res[:, start : start + size] += r.swap_in[index][...].astype(f32)

    heads_slabs = cfg.heads // 2
    spans = range(0, r.w_q.shape[0], 256)

    def unpack_tails():
        part = r.o_part[-1]
        edge = part.shape[1] - 64
        for slot in range(2 * chips):
            low_half, high_half = slice(0, 64), slice(64, 128)
            at = slot * q_block
            r.w_q[at : at + upper, full:] = r.tails[slot, :upper, low_half]
            r.w_q[at + upper : at + q_block, full:] = r.tails[slot, : q_block - upper, high_half]
            at = slot * o_block
            part[at : at + lower, edge:] = r.tails[slot, upper:, low_half]
            part[at + lower : at + o_block, edge:] = r.tails[slot, upper:, high_half]

    advance(0, 1)
    advance(1, 1)
    own_sends(2)
    for step in range(2, hops):
        advance(0, step)
        advance(1, step)
        advance(2, step - 1)
    own_sends(3)
    advance(0, hops)
    advance(1, hops)
    all_here(0)
    all_here(1)
    unpack_tails()
    for start in spans[:3]:
        project(start)
    advance(2, hops - 1)
    own_sends(4)
    for start in spans[3:]:
        project(start)
    for slab in range(heads_slabs // 2):
        attend(slab)
    advance(3, 1)
    for slab in range(heads_slabs // 2, heads_slabs):
        attend(slab)
    advance(2, hops)
    advance(4, 1)
    all_here(2)
    swap(0)
    advance(3, 2)
    advance(4, 2)
    advance(3, 3)
    receive(0)
    r.rows_a[me] = r.res[:, :cut].astype(bf16)
    early, late = (0, half // 4), (half // 2, 3 * half // 4)
    own_sends(fast, early, False)
    advance(4, 3)
    own_sends(fast, late)
    advance(3, 4)
    all_here(3)
    swap(1)
    advance(fast, 1, early)
    advance(4, 4)
    all_here(4)
    swap(2)
    advance(fast, 1, late)
    receive(1)
    advance(fast, 2)
    receive(2)

    experts = router.shape[0]
    top_count = cfg.top_count
    residual = r.res[...]
    mean_sq = jnp.mean(residual * residual, axis=-1, keepdims=True)
    scale = lax.rsqrt(mean_sq + norm_eps)
    head = (r.res[:, :cut] * scale * mlp[:cut][None, :]).astype(bf16)
    tail = (r.res[:, cut:] * scale * mlp[cut:][None, :]).astype(bf16)
    r.rows_b[me] = tail
    edge = tail.shape[1] - 64
    quiet = r.notes.shape[1] - half // 2
    r.notes[me, quiet:, :64] = tail[: half // 2, edge:]
    r.notes[me, quiet:, 64:] = tail[half // 2 :, edge:]
    across_lanes = (((1,), (1,)), ((), ()))
    logits = (
        lax.dot_general(router[:, :cut], head, across_lanes, preferred_element_type=f32)
        + lax.dot_general(router[:, cut:], tail, across_lanes, preferred_element_type=f32)
        + jnp.transpose(jnp.broadcast_to(bias[...], (half, experts)))
    )
    ids = ids_ref[:, ours]
    expert = lax.broadcasted_iota(jnp.int32, (experts, half), 0)
    picked = [ids[k : k + 1, :] == expert for k in range(top_count)]
    hit = sum(jnp.where(p, 1.0, 0.0) for p in picked)
    earlier = lax.broadcasted_iota(jnp.int32, (half, half), 0) < lax.broadcasted_iota(
        jnp.int32, (half, half), 1
    )
    before = jnp.dot(
        hit.astype(bf16), jnp.where(earlier, 1.0, 0.0).astype(bf16), preferred_element_type=f32
    )
    raised = [jnp.exp(jnp.sum(jnp.where(p, logits, 0.0), axis=0, keepdims=True)) for p in picked]
    share = 1.0 / sum(raised)
    line = lax.broadcasted_iota(jnp.int32, (quiet, half), 0)
    note = jnp.zeros(line.shape, f32)
    for k in range(top_count):
        slot = jnp.sum(jnp.where(picked[k], before, 0.0), axis=0, keepdims=True)
        note = jnp.where(line == k, raised[k] * share, note)
        note = jnp.where(line == top_count + k, ids[k : k + 1, :].astype(f32), note)
        note = jnp.where(line == 2 * top_count + k, slot, note)
    rest = jnp.transpose(jnp.broadcast_to(scale, (half, 128)))[:1, :]
    for k in range(3):
        term = rest.astype(bf16).astype(f32)
        note = jnp.where(line == 3 * top_count + k, term, note)
        rest = rest - term
    r.notes[me, :quiet] = note.astype(bf16)

    def take(slot):
        own_expert = me.astype(f32)
        note = r.notes[slot, :quiet].astype(f32)
        r.rows_b[slot, : half // 2, edge:] = r.notes[slot, quiet:, :64]
        r.rows_b[slot, half // 2 :, edge:] = r.notes[slot, quiet:, 64:]
        gate = jnp.zeros((1, half), f32)
        where_to = jnp.full((1, half), -1.0, f32)
        for k in range(top_count):
            chosen = note[top_count + k : top_count + k + 1, :] == own_expert
            gate = jnp.where(chosen, note[k : k + 1, :], gate)
            where_to = jnp.where(chosen, note[2 * top_count + k : 2 * top_count + k + 1, :], where_to)
        at = 3 * top_count
        scales = note[at : at + 1, :] + note[at + 1 : at + 2, :] + note[at + 2 : at + 3, :]
        match = lax.broadcasted_iota(jnp.int32, (capacity, half), 0).astype(f32) == where_to
        select = jnp.where(match, 1.0, 0.0).astype(bf16)
        gates = lax.dot_general(
            jnp.broadcast_to(gate, (8, half)).astype(bf16), select, across_lanes,
            preferred_element_type=f32,
        )
        r.gate_rows[slot] = gates[:1, :]
        scales = jnp.sum(jnp.where(match, scales, 0.0), axis=1, keepdims=True)
        r.out[slot, :, cut:] = jnp.dot(
            select, r.rows_b[slot], preferred_element_type=f32
        ).astype(bf16)
        r.out[slot, :, :cut] = (
            jnp.dot(select, r.rows_a[slot], preferred_element_type=f32)
            * scales * mlp[:cut][None, :]
        ).astype(bf16)

    own_sends(marks)
    own_sends(slow)
    advance(fast, 3)
    take(me)

    def ring_task(way, step):
        return lambda: take(origin(way, step))

    def pair_task(ways, step):
        def run():
            for group in (fast, slow, marks):
                pair_wait(group, ways[0], step)
            take(origin(ways[0], step) + flip)
        return run

    def partner_task():
        for group in (fast, slow, marks):
            pair_wait(group, 1, 0)
        take(partner)

    tasks.append(partner_task)
    for step in range(1, hops + 1):
        advance(marks, step)
        advance(slow, step)
        if step == 1:
            advance(fast, 4)
        for ways in ((1,), (-1,)) if step < hops else ((1, -1),):
            tasks.append(ring_task(ways[0], step))
            tasks.append(pair_task(ways, step))
    while tasks:
        tasks.pop(0)()
    r.gates[...] = r.gate_rows[:, 0, :].astype(bf16)

    for group in range(marks + 1):
        landed(blocks(group, chips - 1), r.ring_send.at[group])
        landed(blocks(group, chips), r.pair_send.at[group])
    for index in range(swaps):
        swap_copy(index).wait_send()


def write_kernel(pieces, out_ref, gate_ref, out_hbm, gate_hbm, sems):
    share = out_ref.shape[0] // pieces
    copies = [pltpu.make_async_copy(gate_ref, gate_hbm, sems.at[pieces])]
    for piece in range(pieces):
        part = pl.ds(piece * share, share)
        copies.append(pltpu.make_async_copy(out_ref.at[part], out_hbm.at[part], sems.at[piece]))
    for copy in copies:
        copy.start()
    for copy in copies:
        copy.wait()


def write_call(out, gates, pieces):
    vmem, hbm = (pl.BlockSpec(memory_space=kind) for kind in (pltpu.VMEM, pltpu.HBM))
    return pl.pallas_call(
        functools.partial(write_kernel, pieces),
        out_shape=[pltpu.HBM(v.shape, v.dtype) for v in (out, gates)],
        in_specs=[vmem] * 2,
        out_specs=[hbm] * 2,
        scratch_shapes=[pltpu.SemaphoreType.DMA((pieces + 1,))],
        compiler_params=pltpu.CompilerParams(vmem_limit_bytes=2 * 1024 * 1024),
        name="write_out",
    )(out, gates)


def layer_call(
    tokens, segments, expert_ids, gain, sinks, adam, router_weight, router_bias, mlp_gain,
    heads, kv_heads, sources, experts, capacity,
):
    rows, width = tokens.shape
    half = rows // 2
    chips = sources // 2
    hops = chips // 2
    q_block, o_block = adam[0].shape[0], adam[4].shape[0]
    top_count = expert_ids.shape[1]
    cut = width * 3 // 8 // 128 * 128
    segments_o = ((0, cut), (cut, cut), (2 * cut, width - 2 * cut))
    tiles = q_block // 16
    top = (tiles + 1) // 2 * 16
    q_spans = [(0, 16, 1), (16, top - 16, 1), (top, q_block - top, -1)]
    o_spans = [(0, o_block // 2, 1), (o_block // 2, o_block // 2, -1)]
    last_spans = [(0, 16, 1), (16, o_block - 16, -1)]
    quarter = half // 4
    r_spans = [(quarter * t, quarter, 1 if t < 2 else -1) for t in range(4)]
    tops = (q_block + 31) // 32 * 16, o_block // 2
    tail_rows, note_rows = sum(tops), 16 + half // 2

    spans = (
        q_spans, [(0, tail_rows, -1)], o_spans, o_spans, last_spans, r_spans, r_spans,
        [(0, note_rows, 1)],
    )
    plan, total = piece_plan(spans, hops)
    cosine, sine = split_tables(rows)
    bf16, f32 = jnp.bfloat16, jnp.float32
    hbm = dict(
        tok=tokens.T, adam=adam,
        small=[
            gain, mlp_gain, segments[None, :], jnp.asarray(cosine), jnp.asarray(sine),
            router_weight.T, router_bias[None, :], expert_ids.T, sinks,
        ],
    )
    small = [pltpu.VMEM(v.shape, v.dtype) for v in hbm["small"][:-1]]
    dma = pltpu.SemaphoreType.DMA
    groups, swaps = len(spans), len(segments_o)
    scratch = dict(
        tok=pltpu.VMEM(tokens.shape, bf16),
        tok_t=pltpu.VMEM((width, rows), bf16),
        small=small + [pltpu.SMEM(sinks.shape, sinks.dtype)],
        mask=pltpu.VMEM((rows, rows), f32),
        q_in=pltpu.VMEM((4, q_block, width), f32),
        o_in=pltpu.VMEM((4, o_block, width), f32),
        normed=pltpu.VMEM((rows, width), bf16),
        w_q=pltpu.VMEM((sources * q_block, width), bf16),
        tails=pltpu.VMEM((sources, tail_rows, 128), bf16),
        o_part=[pltpu.VMEM((sources * o_block, size), bf16) for _, size in segments_o],
        proj=pltpu.VMEM((rows, sources * q_block), f32),
        att=pltpu.VMEM((rows, heads * HEAD_DIM), bf16),
        res=pltpu.VMEM((half, width), f32),
        swap_out=[pltpu.VMEM((half, size), bf16) for _, size in segments_o],
        swap_in=[pltpu.VMEM((half, size), bf16) for _, size in segments_o],
        rows_a=pltpu.VMEM((sources, half, cut), bf16),
        rows_b=pltpu.VMEM((sources, half, width - cut), bf16),
        notes=pltpu.VMEM((sources, note_rows, half), bf16),
        gate_rows=pltpu.VMEM((sources, 1, capacity), f32),
        load_sem=dma((tiles + 11,)),
        ring_send=dma((groups,)),
        ring_recv=dma((total,)),
        pair_send=dma((groups,)),
        pair_recv=dma((groups - 3 + 3 * chips,)),
        swap_send=dma((swaps,)),
        swap_recv=dma((swaps,)),
    )
    results = dict(
        out=pltpu.VMEM((sources, capacity, width), bf16),
        gates=pltpu.VMEM((sources, capacity), bf16),
    )
    operands, hbm_tree = jax.tree.flatten(hbm)
    outputs, result_tree = jax.tree.flatten(results)
    buffers, scratch_tree = jax.tree.flatten(scratch)
    own = (q_block, tail_rows, *[o_block] * swaps, half, half, note_rows)
    cfg = types.SimpleNamespace(
        plan=plan, own=own, chips=chips, heads=heads, kv_heads=kv_heads, segments=segments_o,
        top_count=top_count, tops=tops,
    )

    def body(*refs):
        taken = list(refs)
        spaces = []
        for tree in (hbm_tree, result_tree, scratch_tree):
            count = tree.num_leaves
            spaces.append(jax.tree.unflatten(tree, taken[:count]))
            taken = taken[count:]
        layer_kernel(
            cfg, types.SimpleNamespace(**spaces[0]),
            types.SimpleNamespace(**spaces[1], **spaces[2]),
        )

    gates, out = pl.pallas_call(
        body,
        out_shape=outputs,
        in_specs=[pl.BlockSpec(memory_space=pltpu.HBM)] * len(operands),
        out_specs=[pl.BlockSpec(memory_space=pltpu.VMEM)] * 2,
        scratch_shapes=buffers,
        compiler_params=pltpu.CompilerParams(
            collective_id=4, has_side_effects=True, vmem_limit_bytes=48 * 1024 * 1024
        ),
        name="layer",
    )(*(pltpu.with_memory_space_constraint(v, pltpu.HBM) for v in operands))
    return write_call(out, gates, 8)


def layer_fits(tokens, adam, sources, experts, capacity, groups):
    rows, width = tokens.shape
    return (
        groups == 2 and experts == sources and sources == 16 and rows == 256
        and adam[0].shape[0] % 16 == 0 and adam[0].shape[0] >= 80 and adam[4].shape[0] % 32 == 0
        and width % 128 == 64 and width >= 1024 and capacity <= 128
    )


def on_device(
    tokens,
    segment_ids,
    expert_ids,
    attn_gain,
    sinks,
    qkv_master,
    qkv_mom,
    qkv_var,
    qkv_grad,
    o_master,
    o_mom,
    o_var,
    o_grad,
    router_weight,
    router_bias,
    mlp_gain,
):
    tok_rows, width = tokens.shape
    half = tok_rows // lax.axis_size("dp")
    sources = lax.axis_size("expert")
    heads_here = sinks.shape[0]
    kv_here = KV_HEADS * heads_here // HEADS
    experts = router_weight.shape[1]
    top_count = expert_ids.shape[1]
    capacity = 2 * half * top_count // experts
    adam = [qkv_master, qkv_mom, qkv_var, qkv_grad, o_master, o_mom, o_var, o_grad]
    if layer_fits(tokens, adam, sources, experts, capacity, lax.axis_size("dp")):
        dispatched, gate_slots = layer_call(
            tokens, segment_ids, expert_ids, attn_gain, sinks, adam, router_weight, router_bias,
            mlp_gain, heads_here, kv_here, sources, experts, capacity,
        )
        return (dispatched[None, :, None], gate_slots[None, :, None])
    qkv_local = adam_weights(qkv_master, qkv_mom, qkv_var, qkv_grad)
    o_local = adam_weights(o_master, o_mom, o_var, o_grad)
    qkv_full, o_full = gather_rows([qkv_local, o_local], sources, 1)
    part = attention_call(
        tokens, attn_gain, qkv_full, o_full, segment_ids, sinks, heads_here, kv_here
    ).reshape(-1, half, width)
    got = exchange_call(part, 2)
    rows = router_call(
        tokens, part, got, mlp_gain, router_weight, router_bias, expert_ids, 128 - width % 128
    )
    compact = sources * half <= 2 * experts * capacity
    if experts == sources and compact and ring_fits([rows], sources):
        dispatched, gate_slots = ring_gather(
            [rows], 4, sources, 3, (top_count, capacity, width)
        )
        return (dispatched[None, :, None], gate_slots[None])
    return exchange_slots(rows, width, experts, capacity, top_count, sources)


def solution(mesh):
    return jax.shard_map(
        on_device,
        mesh=mesh,
        in_specs=(
            P("expert", None),
            P("expert"),
            P("expert", None),
            P(),
            P("dp"),
            P(("dp", "expert"), None),
            P(("dp", "expert"), None),
            P(("dp", "expert"), None),
            P(("dp", "expert"), None),
            P(("dp", "expert"), None),
            P(("dp", "expert"), None),
            P(("dp", "expert"), None),
            P(("dp", "expert"), None),
            P(),
            P(),
            P(),
        ),
        out_specs=(P("expert", None, "dp", None, None), P("expert", None, "dp", None)),
        check_vma=False,
    )
```
